16 devices in a mesh: dp: 2 (over y, z), tp: 8 (over x, core).
Axes of the slice: x: 4, y: 2, z: 1, core: 2. Of those that a mesh axis runs over, the one named last changes fastest.
The devices are a block of a 4x4x8 slice.
Arguments:
- x: bfloat16 [2048, 1024], P('dp'), parts along dimension 0
- k_cache: bfloat16 [2048, 64, 16, 64], P('dp', None, 'tp'), parts along dimension 0
- v_cache: bfloat16 [2048, 64, 16, 64], P('dp', None, 'tp'), parts along dimension 0
- positions: int32 [2048], P('dp'), parts along dimension 0
- att_ids: int32 [2048, 2], P('dp'), parts along dimension 0
- mlp_ids: int32 [2048, 2], P('dp'), parts along dimension 0
- norm_att: float32 [1024], replicated
- w_kv: bfloat16 [1024, 16, 128], P(None, 'tp')
- router_att: bfloat16 [1024, 16], replicated
- w_query: bfloat16 [16, 1024, 1024], P(None, None, 'tp')
- w_out: bfloat16 [16, 1024, 1024], P(None, 'tp')
- norm_mlp: float32 [1024], replicated
- router_mlp: bfloat16 [1024, 32], replicated
- w_gate: bfloat16 [32, 1024, 2048], P('tp')
- w_up: bfloat16 [32, 1024, 2048], P('tp')
- w_down: bfloat16 [32, 2048, 1024], P('tp')
Outputs:
- output 1: bfloat16 [2048, 1024], P('dp'), parts along dimension 0
- output 2: bfloat16 [2048, 64, 16, 64], P('dp', None, 'tp'), parts along dimension 0
- output 3: bfloat16 [2048, 64, 16, 64], P('dp', None, 'tp'), parts along dimension 0
There are 2 independent parts. The reference program is written for one: setup_inputs(seed, part) draws one part's arguments, and reference() takes and returns one part's arrays. A program takes and returns all parts, laid end to end along the dimension named above; an argument that names none is the same for every part.
All inputs are finite; a program needn't handle non-finite values.
Results may differ from the reference program's by a relative error of at most 0.01323.
Values are sent between devices in bfloat16 or wider.
A program may use at most 768 MiB of HBM per device.

```python
import jax
import jax.numpy as jnp
from jax import lax

HIDDEN = 1024
KV_HEADS = 16
HEAD_DIM = 64
ATT_EXPERTS = 16
MLP_EXPERTS = 32
FFN_WIDTH = 2048
TOKENS = 1024
CACHE_LEN = 64

QUERY_WIDTH = KV_HEADS * HEAD_DIM
NORM_EPS = 1e-6
ROPE_BASE = 10000.0


def draw_pair(base_key, experts, skewed):
    key_first, key_offset, key_hot, key_share, key_coin = jax.random.split(base_key, 5)
    first_pick = jax.random.randint(key_first, (TOKENS,), 0, experts)
    if skewed:
        hot_id = jax.random.randint(key_hot, (), 0, experts)
        hot_share = jax.random.randint(key_share, (), 40, 61)
        coin_flip = jax.random.randint(key_coin, (TOKENS,), 0, 100)
        first_pick = jnp.where(coin_flip < hot_share, hot_id, first_pick)
    offset = jax.random.randint(key_offset, (TOKENS,), 1, experts)
    token_index = jnp.arange(TOKENS)
    forced = (token_index < experts) & (token_index != first_pick)
    second_pick = jnp.where(forced, token_index, (first_pick + offset) % experts)
    return jnp.stack([first_pick, second_pick], axis=1).astype(jnp.int32)


def draw_positions(base_key):
    positions = jax.random.randint(base_key, (TOKENS,), CACHE_LEN // 4, CACHE_LEN)
    return positions.at[0].set(CACHE_LEN - 1).at[1].set(CACHE_LEN // 4).astype(jnp.int32)


def setup_inputs(seed: int = 0, part: int = 0) -> dict:
    shared_keys = jax.random.split(jax.random.key(seed), 10)
    part_keys = jax.random.split(jax.random.fold_in(jax.random.key(seed + 1), part), 6)
    cache_shape = (TOKENS, CACHE_LEN, KV_HEADS, HEAD_DIM)
    x = jax.random.normal(part_keys[0], (TOKENS, HIDDEN), jnp.float32).astype(jnp.bfloat16)
    k_cache = jax.random.normal(part_keys[1], cache_shape, jnp.float32).astype(jnp.bfloat16)
    value_mean = jax.random.normal(part_keys[2], (TOKENS, 1, KV_HEADS, HEAD_DIM), jnp.float32)
    value_noise = jax.random.normal(part_keys[3], cache_shape, jnp.float32)
    v_cache = (0.8 * value_mean + 0.6 * value_noise).astype(jnp.bfloat16)
    positions = draw_positions(part_keys[4])
    choice_keys = jax.random.split(part_keys[5], 2)
    att_ids = draw_pair(choice_keys[0], ATT_EXPERTS, False)
    mlp_ids = draw_pair(choice_keys[1], MLP_EXPERTS, True)
    norm_att = 1.0 + 0.3 * jax.random.normal(shared_keys[0], (HIDDEN,), jnp.float32)
    w_kv = (jax.random.normal(shared_keys[1], (HIDDEN, KV_HEADS, 2 * HEAD_DIM), jnp.float32) * HIDDEN ** -0.5).astype(jnp.bfloat16)
    router_att = (jax.random.normal(shared_keys[2], (HIDDEN, ATT_EXPERTS), jnp.float32) * 0.5 * HIDDEN ** -0.5).astype(jnp.bfloat16)
    w_query = (jax.random.normal(shared_keys[3], (ATT_EXPERTS, HIDDEN, QUERY_WIDTH), jnp.float32) * HIDDEN ** -0.5).astype(jnp.bfloat16)
    w_out = (jax.random.normal(shared_keys[4], (ATT_EXPERTS, QUERY_WIDTH, HIDDEN), jnp.float32) * QUERY_WIDTH ** -0.5).astype(jnp.bfloat16)
    norm_mlp = 1.0 + 0.3 * jax.random.normal(shared_keys[5], (HIDDEN,), jnp.float32)
    router_mlp = (jax.random.normal(shared_keys[6], (HIDDEN, MLP_EXPERTS), jnp.float32) * 0.5 * HIDDEN ** -0.5).astype(jnp.bfloat16)
    w_gate = (jax.random.normal(shared_keys[7], (MLP_EXPERTS, HIDDEN, FFN_WIDTH), jnp.float32) * HIDDEN ** -0.5).astype(jnp.bfloat16)
    w_up = (jax.random.normal(shared_keys[8], (MLP_EXPERTS, HIDDEN, FFN_WIDTH), jnp.float32) * HIDDEN ** -0.5).astype(jnp.bfloat16)
    w_down = (jax.random.normal(shared_keys[9], (MLP_EXPERTS, FFN_WIDTH, HIDDEN), jnp.float32) * FFN_WIDTH ** -0.5).astype(jnp.bfloat16)
    return {'x': x, 'k_cache': k_cache, 'v_cache': v_cache, 'positions': positions, 'att_ids': att_ids, 'mlp_ids': mlp_ids, 'norm_att': norm_att, 'w_kv': w_kv, 'router_att': router_att, 'w_query': w_query, 'w_out': w_out, 'norm_mlp': norm_mlp, 'router_mlp': router_mlp, 'w_gate': w_gate, 'w_up': w_up, 'w_down': w_down}


def rms_norm(x, gain):
    values = x.astype(jnp.float32)
    inv_rms = lax.rsqrt(jnp.mean(values * values, axis=-1, keepdims=True) + NORM_EPS)
    return (values * inv_rms * gain).astype(jnp.bfloat16)


def rope_tables(positions):
    half_dim = HEAD_DIM // 2
    inv_freq = ROPE_BASE ** (-(jnp.arange(half_dim, dtype=jnp.float32) * 2.0 / HEAD_DIM))
    angles = positions.astype(jnp.float32)[:, None] * inv_freq[None, :]
    return jnp.cos(angles), jnp.sin(angles)


def apply_rope(vectors, cos_table, sin_table):
    half_dim = vectors.shape[-1] // 2
    first_half = vectors[..., :half_dim]
    second_half = vectors[..., half_dim:]
    return jnp.concatenate([first_half * cos_table - second_half * sin_table, second_half * cos_table + first_half * sin_table], axis=-1)


def reference(x, k_cache, v_cache, positions, att_ids, mlp_ids, norm_att, w_kv, router_att, w_query, w_out, norm_mlp, router_mlp, w_gate, w_up, w_down):
    hidden = rms_norm(x, norm_att)
    kv_new = jnp.dot(hidden, w_kv.reshape(HIDDEN, KV_HEADS * 2 * HEAD_DIM), preferred_element_type=jnp.float32).reshape(TOKENS, KV_HEADS, 2 * HEAD_DIM)
    cos_table, sin_table = rope_tables(positions)
    key_new = apply_rope(kv_new[:, :, :HEAD_DIM], cos_table[:, None, :], sin_table[:, None, :]).astype(jnp.bfloat16)
    value_new = kv_new[:, :, HEAD_DIM:].astype(jnp.bfloat16)
    slot_index = jnp.arange(CACHE_LEN)
    at_slot = (slot_index[None, :] == positions[:, None])[:, :, None, None]
    keys_all = jnp.where(at_slot, key_new[:, None, :, :], k_cache)
    values_all = jnp.where(at_slot, value_new[:, None, :, :], v_cache)
    att_logits = jnp.dot(hidden, router_att, preferred_element_type=jnp.float32)
    att_gates = jax.nn.softmax(jnp.take_along_axis(att_logits, att_ids, axis=1), axis=-1)
    query_all = jnp.einsum('bd,edc->bec', hidden.astype(jnp.float32), w_query.astype(jnp.float32))
    query_sel = jnp.take_along_axis(query_all, att_ids[:, :, None], axis=1).reshape(TOKENS, 2, KV_HEADS, HEAD_DIM)
    query_rot = apply_rope(query_sel, cos_table[:, None, None, :], sin_table[:, None, None, :]).astype(jnp.bfloat16)
    scores = jnp.einsum('bknd,bsnd->bkns', query_rot.astype(jnp.float32), keys_all.astype(jnp.float32)) * HEAD_DIM ** -0.5
    visible = (slot_index[None, :] <= positions[:, None])[:, None, None, :]
    weights = jax.nn.softmax(jnp.where(visible, scores, -1e30), axis=-1).astype(jnp.bfloat16)
    attended = jnp.einsum('bkns,bsnd->bknd', weights.astype(jnp.float32), values_all.astype(jnp.float32)).astype(jnp.bfloat16).reshape(TOKENS, 2, QUERY_WIDTH)
    att_onehot = (att_ids[:, :, None] == jnp.arange(ATT_EXPERTS)[None, None, :]).astype(jnp.float32)
    out_slots = jnp.einsum('bke,bkc->bec', att_onehot, attended.astype(jnp.float32))
    projected = jnp.einsum('bec,ecd->bed', out_slots, w_out.astype(jnp.float32))
    att_dense = jnp.einsum('bke,bk->be', att_onehot, att_gates)
    att_sum = jnp.einsum('be,bed->bd', att_dense, projected)
    x_mid = (x.astype(jnp.float32) + att_sum).astype(jnp.bfloat16)
    normed = rms_norm(x_mid, norm_mlp)
    mlp_logits = jnp.dot(normed, router_mlp, preferred_element_type=jnp.float32)
    mlp_gates = jax.nn.softmax(jnp.take_along_axis(mlp_logits, mlp_ids, axis=1), axis=-1)
    mlp_onehot = (mlp_ids[:, :, None] == jnp.arange(MLP_EXPERTS)[None, None, :]).astype(jnp.float32)
    mlp_dense = jnp.einsum('bke,bk->be', mlp_onehot, mlp_gates)

    def expert_step(running_sum, expert_inputs):
        gate_mat, up_mat, down_mat, weight_col = expert_inputs
        gate_val = jnp.dot(normed, gate_mat, preferred_element_type=jnp.float32)
        up_val = jnp.dot(normed, up_mat, preferred_element_type=jnp.float32)
        activation = (jax.nn.silu(gate_val) * up_val).astype(jnp.bfloat16)
        down_out = jnp.dot(activation, down_mat, preferred_element_type=jnp.float32)
        return running_sum + weight_col[:, None] * down_out, None

    mlp_sum, _ = lax.scan(expert_step, jnp.zeros((TOKENS, HIDDEN), jnp.float32), (w_gate, w_up, w_down, mlp_dense.T))
    x_out = (x_mid.astype(jnp.float32) + mlp_sum).astype(jnp.bfloat16)
    return x_out, keys_all, values_all
```

```python
import functools

import jax
import jax.numpy as jnp
from jax import lax
from jax.experimental import pallas as pl
from jax.experimental.pallas import tpu as pltpu
from jax.sharding import PartitionSpec as P

NORM_EPS = 1e-6
ROPE_BASE = 10000.0
F32 = jnp.float32
BF16 = jnp.bfloat16
MESH = pl.DeviceIdType.MESH


NEG = -1e30


def attn_kernel(x_ref, gain_ref, wkv_ref, router_ref, wq_ref, wo_ref, pos_ref, ids_ref, cos_ref, sin_ref, k_ref, v_ref, part_ref, ko_ref, vo_ref, sc_ref, sel_ref):
    block, width = x_ref.shape
    slots, heads, dim, _ = k_ref.shape
    experts = wq_ref.shape[0]
    cols = heads * dim
    half = dim // 2
    xf = x_ref[...].astype(F32)
    inv = lax.rsqrt(jnp.mean(xf * xf, axis=-1, keepdims=True) + NORM_EPS)
    hidden = (xf * inv * gain_ref[...]).astype(BF16)
    cos_t = cos_ref[...]
    sin_t = sin_ref[...]

    def rope(head):
        first, second = head[:half], head[half:]
        return jnp.concatenate([first * cos_t - second * sin_t, second * cos_t + first * sin_t], axis=0)

    kv_t = jnp.dot(hidden, wkv_ref[...], preferred_element_type=F32).T
    k_new = [rope(kv_t[n * 2 * dim:n * 2 * dim + dim]).astype(BF16) for n in range(heads)]
    v_new = [kv_t[n * 2 * dim + dim:(n + 1) * 2 * dim].astype(BF16) for n in range(heads)]

    logits = lax.dot_general(router_ref[...], hidden, (((1,), (1,)), ((), ())), preferred_element_type=F32)
    ids_row = [ids_ref[j:j + 1, :] for j in range(2)]
    expert_iota = lax.broadcasted_iota(jnp.int32, (experts, block), 0)
    picked = [jnp.sum(jnp.where(expert_iota == ids_row[j], logits, 0.0), axis=0, keepdims=True) for j in range(2)]
    top = jnp.maximum(picked[0], picked[1])
    raised = [jnp.exp(p - top) for p in picked]
    gate = [r / (raised[0] + raised[1]) for r in raised]
    ids_col = [jnp.broadcast_to(ids_row[j], (cols, block)).T for j in range(2)]
    gate_col = [jnp.broadcast_to(gate[j], (cols, block)).T for j in range(2)]

    chosen = [jnp.zeros((block, cols), F32) for _ in range(2)]
    for e in range(experts):
        q_e = jnp.dot(hidden, wq_ref[e], preferred_element_type=F32)
        chosen = [jnp.where(ids_col[j] == e, q_e, chosen[j]) for j in range(2)]
    q_rot = []
    for j in range(2):
        q_t = chosen[j].T
        q_rot.append([rope(q_t[n * dim:(n + 1) * dim]).astype(BF16).astype(F32) for n in range(heads)])

    pos = pos_ref[...]
    pos16 = jnp.broadcast_to(pos.astype(F32), (dim, block)).astype(BF16)

    def score_step(s, carry):
        at_slot = pos16 == jnp.full((dim, block), s, jnp.int32).astype(F32).astype(BF16)
        for n in range(heads):
            packed = k_ref[s, n]
            keys = packed.astype(F32)
            for j in range(2):
                sc_ref[j * heads + n, pl.ds(s, 1), :] = jnp.sum(q_rot[j][n] * keys, axis=0, keepdims=True)
            ko_ref[s, n] = jnp.where(at_slot, k_new[n], packed)
        return carry

    lax.fori_loop(0, slots, score_step, 0, unroll=4)

    slot_iota = lax.broadcasted_iota(jnp.int32, (slots, block), 0)
    here = slot_iota == pos
    visible = slot_iota <= pos
    out = []
    for j in range(2):
        for n in range(heads):
            fresh = jnp.sum(q_rot[j][n] * k_new[n].astype(F32), axis=0, keepdims=True)
            score = jnp.where(here, fresh, sc_ref[j * heads + n]) * dim ** -0.5
            score = jnp.where(visible, score, NEG)
            raised_s = jnp.exp(score - jnp.max(score, axis=0, keepdims=True))
            prob = (raised_s / jnp.sum(raised_s, axis=0, keepdims=True)).astype(BF16).astype(F32)
            own = jnp.sum(jnp.where(here, prob, 0.0), axis=0, keepdims=True)
            sc_ref[j * heads + n] = jnp.where(here, 0.0, prob)
            out.append(own * v_new[n].astype(F32))

    def value_step(s, carry):
        at_slot = pos16 == jnp.full((dim, block), s, jnp.int32).astype(F32).astype(BF16)
        carry = list(carry)
        for n in range(heads):
            packed = v_ref[s, n]
            values = packed.astype(F32)
            for j in range(2):
                i = j * heads + n
                carry[i] = carry[i] + sc_ref[i, pl.ds(s, 1), :] * values
            vo_ref[s, n] = jnp.where(at_slot, v_new[n], packed)
        return tuple(carry)

    out = lax.fori_loop(0, slots, value_step, tuple(out), unroll=4)

    total = None
    for j in range(2):
        o_j = jnp.concatenate(out[j * heads:(j + 1) * heads], axis=0).T
        for e in range(experts):
            sel_ref[:, e * cols:(e + 1) * cols] = jnp.where(ids_col[j] == e, o_j, 0.0).astype(BF16)
        projected = jnp.dot(sel_ref[...], wo_ref[...], preferred_element_type=F32)
        scaled = projected * jnp.concatenate([gate_col[j]] * (width // cols), axis=1)
        total = scaled if total is None else total + scaled
    part_ref[...] = total.astype(BF16)


def attention(x, k_cache, v_cache, positions, att_ids, norm_att, w_kv, router_att, w_query, w_out, block=128):
    tokens, width = x.shape
    _, slots, heads, dim = k_cache.shape
    experts = w_query.shape[0]
    cols = heads * dim
    half = dim // 2
    inv_freq = ROPE_BASE ** (-(jnp.arange(half, dtype=F32) * 2.0 / dim))
    angles = inv_freq[:, None] * positions.astype(F32)[None, :]
    k_t = k_cache.transpose(1, 2, 3, 0)
    v_t = v_cache.transpose(1, 2, 3, 0)
    whole = lambda *shape: pl.BlockSpec(shape, lambda i: (0,) * len(shape), pipeline_mode=pl.Buffered(1))
    lane = lambda rows: pl.BlockSpec((rows, block), lambda i: (0, i))
    cache = pl.BlockSpec((slots, heads, dim, block), lambda i: (0, 0, 0, i))
    row = pl.BlockSpec((block, width), lambda i: (i, 0))
    part, k_out, v_out = pl.pallas_call(
        attn_kernel,
        grid=(tokens // block,),
        in_specs=[row, whole(1, width), whole(width, 2 * cols), whole(experts, width), whole(experts, width, cols), whole(experts * cols, width), lane(1), lane(2), lane(half), lane(half), cache, cache],
        out_specs=[row, cache, cache],
        out_shape=[jax.ShapeDtypeStruct((tokens, width), BF16), jax.ShapeDtypeStruct(k_t.shape, BF16), jax.ShapeDtypeStruct(v_t.shape, BF16)],
        scratch_shapes=[pltpu.VMEM((2 * heads, slots, block), F32), pltpu.VMEM((block, experts * cols), BF16)],
        compiler_params=pltpu.CompilerParams(dimension_semantics=("arbitrary",), vmem_limit_bytes=56 * 1024 * 1024),
        name="attention",
    )(x, norm_att.reshape(1, width), w_kv.reshape(width, 2 * cols), router_att.T, w_query, w_out.reshape(experts * cols, width), positions.reshape(1, tokens), att_ids.T, jnp.cos(angles), jnp.sin(angles), k_t, v_t)
    return part, k_out.transpose(3, 0, 1, 2), v_out.transpose(3, 0, 1, 2)


def reduce_kernel(part_ref, resid_ref, out_ref, pair_in, ring, half_in, full_in, own, pair_sem, sems, d2d_sem):
    rows, width = part_ref.shape
    mine = rows // 2
    chips = lax.axis_size("tp") // 2
    piece = mine // chips
    halfw = width // 2
    me = lax.axis_index("tp")
    core = lax.rem(me, 2)
    chip = me // 2
    other = 1 - core
    right_chip = lax.rem(chip + 1, chips)
    left_chip = lax.rem(chip + chips - 1, chips)
    far_chip = lax.rem(chip + 2, chips)
    partner = {"tp": chip * 2 + other}
    right = {"tp": right_chip * 2 + core}
    left = {"tp": left_chip * 2 + core}

    barrier = pltpu.get_barrier_semaphore()
    for peer in (partner, right, left):
        pl.semaphore_signal(barrier, inc=1, device_id=peer, device_id_type=MESH)
    pl.semaphore_wait(barrier, 3)

    def send(src, dst, sem, peer):
        copy = pltpu.make_async_remote_copy(src_ref=src, dst_ref=dst, send_sem=sem.at[0], recv_sem=sem.at[1], device_id=peer, device_id_type=MESH)
        copy.start()
        return copy

    def block(c, q):
        return pl.ds(pl.multiple_of(c * mine + q * piece, piece), piece)

    lo, hi = pl.ds(0, halfw), pl.ds(halfw, halfw)
    order = (far_chip, right_chip, left_chip, chip)
    swaps = [send(part_ref.at[block(other, q)], pair_in.at[pl.ds(pl.multiple_of(q * piece, piece), piece)], pair_sem.at[i], partner) for i, q in enumerate(order)]

    def paired(q):
        return part_ref[block(core, q), :].astype(F32) + pair_in[pl.ds(pl.multiple_of(q * piece, piece), piece), :].astype(F32)

    swaps[0].wait_recv()
    ring[0] = paired(far_chip).astype(BF16)
    far_r = send(ring.at[0, :, lo], half_in.at[0], sems.at[0], right)
    far_l = send(ring.at[0, :, hi], half_in.at[1], sems.at[1], left)
    swaps[1].wait_recv()
    sum_r = paired(right_chip)
    ring[1, :, halfw:] = sum_r[:, halfw:].astype(BF16)
    plain_r = send(ring.at[1, :, hi], full_in.at[0, :, hi], sems.at[2], right)
    swaps[2].wait_recv()
    sum_l = paired(left_chip)
    ring[2, :, :halfw] = sum_l[:, :halfw].astype(BF16)
    plain_l = send(ring.at[2, :, lo], full_in.at[1, :, lo], sems.at[3], left)
    far_r.wait_recv()
    ring[1, :, :halfw] = (sum_r[:, :halfw] + half_in[0].astype(F32)).astype(BF16)
    added_r = send(ring.at[1, :, lo], full_in.at[0, :, lo], sems.at[4], right)
    far_l.wait_recv()
    ring[2, :, halfw:] = (sum_l[:, halfw:] + half_in[1].astype(F32)).astype(BF16)
    added_l = send(ring.at[2, :, hi], full_in.at[1, :, hi], sems.at[5], left)
    swaps[3].wait_recv()
    base = paired(chip)
    resid = resid_ref[block(core, chip), :].astype(F32)
    mine_rows = block(core, chip)
    plain_r.wait_recv()
    added_l.wait_recv()
    own[:, halfw:] = (resid[:, halfw:] + (base[:, halfw:] + full_in[0, :, halfw:].astype(F32) + full_in[1, :, halfw:].astype(F32))).astype(BF16)
    out_l = send(own.at[:, hi], out_ref.at[mine_rows, hi], sems.at[6], left)
    out_r2 = send(own.at[:, hi], out_ref.at[mine_rows, hi], sems.at[7], right)
    plain_l.wait_recv()
    added_r.wait_recv()
    own[:, :halfw] = (resid[:, :halfw] + (base[:, :halfw] + full_in[0, :, :halfw].astype(F32) + full_in[1, :, :halfw].astype(F32))).astype(BF16)
    out_r = send(own.at[:, lo], out_ref.at[mine_rows, lo], sems.at[8], right)
    out_l2 = send(own.at[:, lo], out_ref.at[mine_rows, lo], sems.at[9], left)
    out_ref[mine_rows, :] = own[...]
    d2d = [send(own, out_ref.at[mine_rows], d2d_sem.at[0], partner)]

    left_rows, right_rows, far_rows = block(core, left_chip), block(core, right_chip), block(core, far_chip)
    out_l.wait_recv()
    fwd_l = send(out_ref.at[right_rows, hi], out_ref.at[right_rows, hi], sems.at[10], left)
    out_r.wait_recv()
    fwd_r = send(out_ref.at[left_rows, lo], out_ref.at[left_rows, lo], sems.at[11], right)
    out_r2.wait_recv()
    d2d.append(send(out_ref.at[left_rows], out_ref.at[left_rows], d2d_sem.at[1], partner))
    out_l2.wait_recv()
    d2d.append(send(out_ref.at[right_rows], out_ref.at[right_rows], d2d_sem.at[2], partner))
    fwd_l.wait_recv()
    fwd_r.wait_recv()
    d2d.append(send(out_ref.at[far_rows], out_ref.at[far_rows], d2d_sem.at[3], partner))
    for copy in swaps + [far_r, far_l, plain_r, plain_l, added_r, added_l, out_l, out_r, out_r2, out_l2, fwd_l, fwd_r]:
        copy.wait_send()
    for copy in d2d:
        copy.wait()


def reduce_add(part, resid, collective_id):
    rows, width = part.shape
    mine = rows // 2
    piece = mine // (lax.axis_size("tp") // 2)
    vmem = pl.BlockSpec(memory_space=pltpu.VMEM)
    return pl.pallas_call(
        reduce_kernel,
        in_specs=[vmem, vmem],
        out_specs=vmem,
        out_shape=jax.ShapeDtypeStruct((rows, width), BF16),
        scratch_shapes=[
            pltpu.VMEM((mine, width), BF16),
            pltpu.VMEM((3, piece, width), BF16),
            pltpu.VMEM((2, piece, width // 2), BF16),
            pltpu.VMEM((2, piece, width), BF16),
            pltpu.VMEM((piece, width), BF16),
            pltpu.SemaphoreType.DMA((4, 2)),
            pltpu.SemaphoreType.DMA((12, 2)),
            pltpu.SemaphoreType.DMA((4, 2)),
        ],
        compiler_params=pltpu.CompilerParams(collective_id=collective_id, has_side_effects=True, vmem_limit_bytes=32 * 1024 * 1024),
        name="reduce_add",
    )(part, resid)


def mlp_kernel(rows, x_ref, gain_ref, router_ref, ids_ref, wg_hbm, wu_hbm, wd_hbm, y_ref, wg, wu, wd, normed, act, acc, rank_ref, gate_ref, rank_col, sem):
    tokens, width = x_ref.shape
    local, _, ffn = wg.shape
    experts = router_ref.shape[0]
    copies = []
    for e in range(local):
        copies.append([pltpu.make_async_copy(src.at[e], dst.at[e], sem.at[e, i]) for i, (src, dst) in enumerate(((wg_hbm, wg), (wu_hbm, wu), (wd_hbm, wd)))])
        for c in copies[-1]:
            c.start()

    step = 128
    for t in range(0, tokens, step):
        xf = x_ref[t:t + step, :].astype(F32)
        inv = lax.rsqrt(jnp.mean(xf * xf, axis=-1, keepdims=True) + NORM_EPS)
        normed[t:t + step, :] = (xf * inv * gain_ref[...]).astype(BF16)
    acc[...] = jnp.zeros_like(acc)

    logits = lax.dot_general(router_ref[...], normed[...], (((1,), (1,)), ((), ())), preferred_element_type=F32)
    ids_row = [ids_ref[j:j + 1, :] for j in range(2)]
    expert_iota = lax.broadcasted_iota(jnp.int32, (experts, tokens), 0)
    picked = [jnp.sum(jnp.where(expert_iota == ids_row[j], logits, 0.0), axis=0, keepdims=True) for j in range(2)]
    top = jnp.maximum(picked[0], picked[1])
    raised = [jnp.exp(p - top) for p in picked]
    gate = [r / (raised[0] + raised[1]) for r in raised]
    first = lax.axis_index("tp") * local
    local_iota = first + lax.broadcasted_iota(jnp.int32, (8, tokens), 0)
    hit = [(ids_row[j] == local_iota) for j in range(2)]
    member = jnp.where(hit[0] | hit[1], 1.0, 0.0)
    gate_ref[...] = jnp.where(hit[0], gate[0], 0.0) + jnp.where(hit[1], gate[1], 0.0)
    tri = jnp.where(lax.broadcasted_iota(jnp.int32, (step, step), 0) <= lax.broadcasted_iota(jnp.int32, (step, step), 1), 1.0, 0.0).astype(BF16)
    running = jnp.zeros((8, 1), F32)
    for t in range(0, tokens, step):
        piece = member[:, t:t + step]
        inside = jnp.dot(piece.astype(BF16), tri, preferred_element_type=F32)
        rank = jnp.where(piece > 0, inside + running - 1.0, -1.0)
        rank_ref[:, t:t + step] = rank
        rank_col[t:t + step, :] = jnp.broadcast_to(rank[:, None, :], (8, step // 8, step)).reshape(step, step).T
        running = running + jnp.sum(piece, axis=1, keepdims=True)

    for e in range(local):
        count = jnp.sum(member[e:e + 1, :]).astype(jnp.int32)
        for c in copies[e][:2]:
            c.wait()
        tiles = (count + rows - 1) // rows
        rank_row = rank_ref[e:e + 1, :]
        gate_row = gate_ref[e:e + 1, :]

        def tile_step(i, down_ready):
            base = (i * rows).astype(F32)
            hits = rank_row == lax.broadcasted_iota(jnp.int32, (rows, tokens), 0).astype(F32) + base
            gate_col = jnp.sum(jnp.where(hits, gate_row, 0.0), axis=1, keepdims=True)
            picked_rows = jnp.dot(jnp.where(hits, 1.0, 0.0).astype(BF16), normed[...], preferred_element_type=F32).astype(BF16)
            for f in range(0, ffn, 512):
                g = jnp.dot(picked_rows, wg[e, :, f:f + 512], preferred_element_type=F32)
                u = jnp.dot(picked_rows, wu[e, :, f:f + 512], preferred_element_type=F32)
                act[:, f:f + 512] = (jax.nn.silu(g) * u).astype(BF16)

            @pl.when(i == 0)
            def _():
                copies[e][2].wait()

            for t in range(0, tokens, 256):
                col = rank_col[t:t + 256, e * (step // 8):e * (step // 8) + 1]
                place = col == lax.broadcasted_iota(jnp.int32, (256, rows), 1).astype(F32) + base
                spread = jnp.where(place, 1.0, 0.0).astype(BF16)
                if t == 0:
                    down = (jnp.dot(act[...], wd[e], preferred_element_type=F32) * gate_col).astype(BF16)
                acc[t:t + 256, :] += jnp.dot(spread, down, preferred_element_type=F32)
            return down_ready

        lax.fori_loop(0, tiles, tile_step, 0)

        @pl.when(tiles == 0)
        def _():
            copies[e][2].wait()

    y_ref[...] = acc[...].astype(BF16)


def experts_mlp(x1, mlp_ids, norm_mlp, router_mlp, w_gate, w_up, w_down, rows=128):
    tokens, width = x1.shape
    local, _, ffn = w_gate.shape
    vmem = pl.BlockSpec(memory_space=pltpu.VMEM)
    hbm = pl.BlockSpec(memory_space=pl.ANY)
    return pl.pallas_call(
        functools.partial(mlp_kernel, rows),
        in_specs=[vmem, vmem, vmem, vmem, hbm, hbm, hbm],
        out_specs=vmem,
        out_shape=jax.ShapeDtypeStruct((tokens, width), BF16),
        scratch_shapes=[
            pltpu.VMEM((local, width, ffn), BF16),
            pltpu.VMEM((local, width, ffn), BF16),
            pltpu.VMEM((local, ffn, width), BF16),
            pltpu.VMEM((tokens, width), BF16),
            pltpu.VMEM((rows, ffn), BF16),
            pltpu.VMEM((tokens, width), F32),
            pltpu.VMEM((8, tokens), F32),
            pltpu.VMEM((8, tokens), F32),
            pltpu.VMEM((tokens, 128), F32),
            pltpu.SemaphoreType.DMA((local, 3)),
        ],
        compiler_params=pltpu.CompilerParams(vmem_limit_bytes=67043328),
        name="experts",
    )(x1, norm_mlp.reshape(1, width), router_mlp.T, mlp_ids.T, w_gate, w_up, w_down)


def solution(mesh):
    def local_step(x, k_cache, v_cache, positions, att_ids, mlp_ids, norm_att, w_kv, router_att, w_query, w_out, norm_mlp, router_mlp, w_gate, w_up, w_down):
        part, keys_all, values_all = attention(x, k_cache, v_cache, positions, att_ids, norm_att, w_kv, router_att, w_query, w_out)
        x_mid = reduce_add(part, x, 0)
        mlp_part = experts_mlp(x_mid, mlp_ids, norm_mlp, router_mlp, w_gate, w_up, w_down)
        x_out = reduce_add(mlp_part, x_mid, 1)
        return x_out, keys_all, values_all

    token_spec = P('dp', None)
    cache_spec = P('dp', None, 'tp', None)
    expert_spec = P('tp', None, None)
    in_specs = (token_spec, cache_spec, cache_spec, P('dp'), token_spec, token_spec, P(), P(None, 'tp', None), P(), P(None, None, 'tp'), P(None, 'tp', None), P(), P(), expert_spec, expert_spec, expert_spec)
    out_specs = (token_spec, cache_spec, cache_spec)
    return jax.shard_map(local_step, mesh=mesh, in_specs=in_specs, out_specs=out_specs, check_vma=False)
```

```python
import functools

import jax
import jax.numpy as jnp
import numpy as np
from jax import lax
from jax.experimental import pallas as pl
from jax.experimental.pallas import tpu as pltpu
from jax.sharding import PartitionSpec as P

NORM_EPS = 1e-6
ROPE_BASE = 10000.0
F32 = jnp.float32
BF16 = jnp.bfloat16
VMEM_LIMIT = 67043328
MESH = pl.DeviceIdType.MESH


NEG = -1e30


def attn_kernel(x_ref, gain_ref, wkv_ref, router_ref, wq_ref, pos_ref, ids_ref, freq_ref, k_ref, v_ref, o_ref, gate_ref, ko_ref, vo_ref, sc_ref, fold_ref, kv_ref):
    block, width = x_ref.shape
    slots, heads, dim, _ = k_ref.shape
    experts = wq_ref.shape[0]
    cols = heads * dim
    half = dim // 2
    xf = x_ref[...].astype(F32)
    inv = lax.rsqrt(jnp.mean(xf * xf, axis=-1, keepdims=True) + NORM_EPS)
    hidden = (xf * inv * gain_ref[...]).astype(BF16)
    pos = pos_ref[...]
    angles = freq_ref[...] * pos.astype(F32)
    cos_t = jnp.cos(angles)
    sin_t = jnp.sin(angles)

    @pl.when(pl.program_id(0) == 0)
    def _():
        for n in range(heads):
            kv_ref[:, n * 2 * dim:(n + 1) * 2 * dim] = wkv_ref[:, n, :]

    def rope(head):
        first, second = head[:half], head[half:]
        return jnp.concatenate([first * cos_t - second * sin_t, second * cos_t + first * sin_t], axis=0)

    kv_t = jnp.dot(hidden, kv_ref[...], preferred_element_type=F32).T
    k_new = [rope(kv_t[n * 2 * dim:n * 2 * dim + dim]).astype(BF16) for n in range(heads)]
    v_new = [kv_t[n * 2 * dim + dim:(n + 1) * 2 * dim].astype(BF16) for n in range(heads)]

    logits = lax.dot_general(router_ref[...], hidden, (((1,), (1,)), ((), ())), preferred_element_type=F32)
    ids_row = [ids_ref[j:j + 1, :] for j in range(2)]
    expert_iota = lax.broadcasted_iota(jnp.int32, (experts, block), 0)
    picked = [jnp.sum(jnp.where(expert_iota == ids_row[j], logits, 0.0), axis=0, keepdims=True) for j in range(2)]
    top = jnp.maximum(picked[0], picked[1])
    raised = [jnp.exp(p - top) for p in picked]
    gate = [r / (raised[0] + raised[1]) for r in raised]
    ids_col = [jnp.broadcast_to(ids_row[j], (cols, block)).T for j in range(2)]
    for j in range(2):
        gate_ref[j:j + 1, :] = gate[j]

    chosen = [jnp.zeros((block, cols), F32) for _ in range(2)]
    for e in range(0, experts, 2):
        q_two = jnp.dot(hidden, jnp.concatenate([wq_ref[e], wq_ref[e + 1]], axis=1), preferred_element_type=F32)
        for i in range(2):
            q_e = q_two[:, i * cols:(i + 1) * cols]
            chosen = [jnp.where(ids_col[j] == e + i, q_e, chosen[j]) for j in range(2)]
    q_rot = []
    for j in range(2):
        q_t = chosen[j].T
        q_rot.append([rope(q_t[n * dim:(n + 1) * dim]).astype(BF16).astype(F32) for n in range(heads)])

    pos16 = jnp.broadcast_to(pos.astype(F32), (dim, block)).astype(BF16)

    def score_step(s, carry):
        at_slot = pos16 == jnp.full((dim, block), s, jnp.int32).astype(F32).astype(BF16)
        for n in range(heads):
            packed = k_ref[s, n]
            keys = packed.astype(F32)
            for j in range(2):
                fold_ref[j * heads + n, pl.ds(pl.multiple_of(s * 8, 8), 8), :] = jnp.sum((q_rot[j][n] * keys).reshape(dim // 8, 8, block), axis=0)
            ko_ref[s, n] = jnp.where(at_slot, k_new[n], packed)
        return carry

    lax.fori_loop(0, slots, score_step, 0, unroll=4)

    slot_iota = lax.broadcasted_iota(jnp.int32, (slots, block), 0)
    here = slot_iota == pos
    visible = slot_iota <= pos
    out = []
    for j in range(2):
        for n in range(heads):
            fresh = jnp.sum(q_rot[j][n] * k_new[n].astype(F32), axis=0, keepdims=True)
            score = fold_ref[j * heads + n, pl.ds(0, slots, stride=8), :]
            for r in range(1, 8):
                score = score + fold_ref[j * heads + n, pl.ds(r, slots, stride=8), :]
            score = jnp.where(here, fresh, score) * dim ** -0.5
            score = jnp.where(visible, score, NEG)
            raised_s = jnp.exp(score - jnp.max(score, axis=0, keepdims=True))
            prob = (raised_s / jnp.sum(raised_s, axis=0, keepdims=True)).astype(BF16).astype(F32)
            own = jnp.sum(jnp.where(here, prob, 0.0), axis=0, keepdims=True)
            sc_ref[j * heads + n] = jnp.where(here, 0.0, prob)
            out.append(own * v_new[n].astype(F32))

    def value_step(s, carry):
        at_slot = pos16 == jnp.full((dim, block), s, jnp.int32).astype(F32).astype(BF16)
        carry = list(carry)
        for n in range(heads):
            packed = v_ref[s, n]
            values = packed.astype(F32)
            for j in range(2):
                i = j * heads + n
                carry[i] = carry[i] + sc_ref[i, pl.ds(s, 1), :] * values
            vo_ref[s, n] = jnp.where(at_slot, v_new[n], packed)
        return tuple(carry)

    out = lax.fori_loop(0, slots, value_step, tuple(out), unroll=4)

    for j in range(2):
        o_ref[j] = jnp.concatenate(out[j * heads:(j + 1) * heads], axis=0).T.astype(BF16)


def attention(x, k_cache, v_cache, positions, att_ids, norm_att, w_kv, router_att, w_query, block=128):
    tokens, width = x.shape
    _, slots, heads, dim = k_cache.shape
    experts = w_query.shape[0]
    cols = heads * dim
    half = dim // 2
    inv_freq = jnp.asarray(ROPE_BASE ** (-(np.arange(half) * 2.0 / dim)), F32)
    k_t = k_cache.transpose(1, 2, 3, 0)
    v_t = v_cache.transpose(1, 2, 3, 0)
    whole = lambda *shape: pl.BlockSpec(shape, lambda i: (0,) * len(shape), pipeline_mode=pl.Buffered(1))
    lane = lambda rows: pl.BlockSpec((rows, block), lambda i: (0, i))
    cache = pl.BlockSpec((slots, heads, dim, block), lambda i: (0, 0, 0, i))
    row = pl.BlockSpec((block, width), lambda i: (i, 0))
    o, gate, k_out, v_out = pl.pallas_call(
        attn_kernel,
        grid=(tokens // block,),
        in_specs=[row, whole(1, width), whole(width, heads, 2 * dim), whole(experts, width), whole(experts, width, cols), lane(1), lane(2), whole(half, 1), cache, cache],
        out_specs=[pl.BlockSpec((2, block, cols), lambda i: (0, i, 0)), lane(2), cache, cache],
        out_shape=[jax.ShapeDtypeStruct((2, tokens, cols), BF16), jax.ShapeDtypeStruct((2, tokens), F32), jax.ShapeDtypeStruct(k_t.shape, BF16), jax.ShapeDtypeStruct(v_t.shape, BF16)],
        scratch_shapes=[pltpu.VMEM((2 * heads, slots, block), F32), pltpu.VMEM((2 * heads, slots * 8, block), F32), pltpu.VMEM((width, 2 * cols), BF16)],
        compiler_params=pltpu.CompilerParams(dimension_semantics=("arbitrary",), vmem_limit_bytes=VMEM_LIMIT),
        name="attention",
    )(x, norm_att.reshape(1, width), w_kv, router_att.T, w_query, positions.reshape(1, tokens), att_ids.T, inv_freq[:, None], k_t, v_t)
    return o, gate, k_out.transpose(3, 0, 1, 2), v_out.transpose(3, 0, 1, 2)


def exchange(produce, loads, resid_hbm, out_ref, stage, pair_in, held, ring, far_in, full_in, own, resid, sel, resid_sem, swap_sem, ring_sem, d2d_sem):
    rows, width = out_ref.shape
    mine = rows // 2
    chips = lax.axis_size("tp") // 2
    piece = mine // chips
    cuts = 4
    cw = width // cuts
    me = lax.axis_index("tp")
    core = lax.rem(me, 2)
    chip = me // 2
    other = 1 - core
    right_chip = lax.rem(chip + 1, chips)
    left_chip = lax.rem(chip + chips - 1, chips)
    far_chip = lax.rem(chip + 2, chips)
    partner = {"tp": chip * 2 + other}
    right = {"tp": right_chip * 2 + core}
    left = {"tp": left_chip * 2 + core}

    barrier = pltpu.get_barrier_semaphore()
    for peer in (partner, right, left):
        pl.semaphore_signal(barrier, inc=1, device_id=peer, device_id_type=MESH)
    for copy in loads:
        copy.start()

    def first_row(c, q):
        return pl.multiple_of(c * mine + q * piece, piece)

    def rows_of(c, q):
        return pl.ds(first_row(c, q), piece)

    resid_copy = pltpu.make_async_copy(resid_hbm.at[rows_of(core, chip)], resid, resid_sem)
    resid_copy.start()
    for copy in loads:
        copy.wait()
    pending = []

    def send(src, dst, sem, peer):
        copy = pltpu.make_async_remote_copy(src_ref=src, dst_ref=dst, send_sem=sem.at[0], recv_sem=sem.at[1], device_id=peer, device_id_type=MESH)
        copy.start()
        pending.append(copy)
        return copy

    def cut(k, n=1):
        return slice(k * cw, (k + n) * cw)

    def dcut(k, n=1):
        return pl.ds(k * cw, n * cw)

    def swap(slot, i, q, k, n):
        stage[slot, :, cut(k, n)] = produce(first_row(other, q), k * cw, n * cw, sel).astype(BF16)
        if i == 0:
            pl.semaphore_wait(barrier, 3)
        copy = send(stage.at[slot, :, dcut(k, n)], pair_in.at[slot, :, dcut(k, n)], swap_sem.at[i], partner)
        held[slot, :, cut(k, n)] = produce(first_row(core, q), k * cw, n * cw, sel)
        return copy

    def land(copy, slot, k, n):
        copy.wait_recv()
        held[slot, :, cut(k, n)] += pair_in[slot, :, cut(k, n)].astype(F32)

    land(swap(0, 0, far_chip, 0, cuts), 0, 0, cuts)
    ring[0] = held[0].astype(BF16)
    far, plain, added = {}, {}, {}
    for k in (0, 2, 1, 3):
        far[k] = send(ring.at[0, :, dcut(k)], far_in.at[:, dcut(k)], ring_sem.at[k], right if k < 2 else left)
    land(swap(1, 1, right_chip, 2, 2), 1, 2, 2)
    ring[1, :, cut(2, 2)] = held[1, :, cut(2, 2)].astype(BF16)
    plain[2] = send(ring.at[1, :, dcut(2)], full_in.at[0, :, dcut(2)], ring_sem.at[6], right)
    land(swap(2, 2, left_chip, 0, 2), 2, 0, 2)
    ring[2, :, cut(0, 2)] = held[2, :, cut(0, 2)].astype(BF16)
    plain[0] = send(ring.at[2, :, dcut(0)], full_in.at[1, :, dcut(0)], ring_sem.at[4], left)
    swap_r = swap(1, 3, right_chip, 0, 2)
    swap_l = swap(2, 4, left_chip, 2, 2)
    land(swap_r, 1, 0, 2)
    land(swap_l, 2, 2, 2)

    def add_on(k):
        slot = 1 if k < 2 else 2
        far[k].wait_recv()
        ring[slot, :, cut(k)] = (held[slot, :, cut(k)] + far_in[:, cut(k)].astype(F32)).astype(BF16)
        added[k] = send(ring.at[slot, :, dcut(k)], full_in.at[slot - 1, :, dcut(k)], ring_sem.at[8 + k], right if k < 2 else left)

    add_on(0)
    add_on(2)
    add_on(1)
    add_on(3)
    plain[3] = send(ring.at[1, :, dcut(3)], full_in.at[0, :, dcut(3)], ring_sem.at[7], right)
    plain[1] = send(ring.at[2, :, dcut(1)], full_in.at[1, :, dcut(1)], ring_sem.at[5], left)
    land(swap(3, 5, chip, 0, cuts), 3, 0, cuts)
    resid_copy.wait()

    own_rows, left_rows, right_rows, far_rows = (rows_of(core, q) for q in (chip, left_chip, right_chip, far_chip))
    to_right, to_left = {}, {}
    for k in (0, 2, 1, 3):
        plain[k].wait_recv()
        added[k].wait_recv()
        own[:, cut(k)] = (resid[:, cut(k)].astype(F32) + (held[3, :, cut(k)] + full_in[0, :, cut(k)].astype(F32) + full_in[1, :, cut(k)].astype(F32))).astype(BF16)
        to_right[k] = send(own.at[:, dcut(k)], out_ref.at[own_rows, dcut(k)], ring_sem.at[12 + k], right)
        to_left[k] = send(own.at[:, dcut(k)], out_ref.at[own_rows, dcut(k)], ring_sem.at[16 + k], left)
    d2d = [send(own, out_ref.at[own_rows], d2d_sem.at[0], partner)]
    out_ref[own_rows, :] = own[...]
    onward = {}
    for k in (0, 2, 1, 3):
        to_right[k].wait_recv()
        if k < 2:
            onward[k] = send(out_ref.at[left_rows, dcut(k)], out_ref.at[left_rows, dcut(k)], ring_sem.at[20 + k], right)
        d2d.append(send(out_ref.at[left_rows, dcut(k)], out_ref.at[left_rows, dcut(k)], d2d_sem.at[1 + k], partner))
        to_left[k].wait_recv()
        if k >= 2:
            onward[k] = send(out_ref.at[right_rows, dcut(k)], out_ref.at[right_rows, dcut(k)], ring_sem.at[20 + k], left)
        d2d.append(send(out_ref.at[right_rows, dcut(k)], out_ref.at[right_rows, dcut(k)], d2d_sem.at[5 + k], partner))
    for k in (0, 2, 1, 3):
        onward[k].wait_recv()
        d2d.append(send(out_ref.at[far_rows, dcut(k)], out_ref.at[far_rows, dcut(k)], d2d_sem.at[9 + k], partner))
    for copy in d2d:
        copy.wait_recv()
    for copy in pending:
        copy.wait_send()


def load_all(pairs, sem):
    return [pltpu.make_async_copy(src, dst, sem.at[i]) for i, (src, dst) in enumerate(pairs)]


def project_kernel(o_hbm, ids_hbm, gate_hbm, wo_hbm, resid_hbm, out_ref, o_ref, ids_ref, gate_ref, wo_ref, load_sem, *rest):
    cols = o_ref.shape[2]
    experts = wo_ref.shape[0] // cols

    def produce(start, col, width, sel):
        block = sel.shape[0]
        total = None
        for j in range(2):
            ids_col = jnp.broadcast_to(ids_ref[j:j + 1, pl.ds(start, block)], (cols, block)).T
            gate_col = jnp.broadcast_to(gate_ref[j:j + 1, pl.ds(start, block)], (cols, block)).T
            o_j = o_ref[j, pl.ds(start, block), :].astype(F32)
            for e in range(experts):
                sel[:, e * cols:(e + 1) * cols] = jnp.where(ids_col == e, o_j, 0.0).astype(BF16)
            projected = jnp.dot(sel[...], wo_ref[:, col:col + width], preferred_element_type=F32)
            scaled = projected * jnp.concatenate([gate_col] * (width // cols), axis=1)
            total = scaled if total is None else total + scaled
        return total

    exchange(produce, load_all(((o_hbm, o_ref), (ids_hbm, ids_ref), (gate_hbm, gate_ref), (wo_hbm, wo_ref)), load_sem), resid_hbm, out_ref, *rest)


def combine_kernel(z_hbm, place_hbm, resid_hbm, out_ref, z_ref, place_ref, load_sem, *rest):
    def produce(start, col, width, sel):
        block = sel.shape[0]
        place = [jnp.broadcast_to(place_ref[j:j + 1, pl.ds(start, block)], (block, block)).T for j in range(2)]
        lane = lax.broadcasted_iota(jnp.int32, (block, block), 1).astype(F32)
        for r in range(0, sel.shape[1], block):
            here = lane + float(r)
            sel[:, r:r + block] = jnp.where((place[0] == here) | (place[1] == here), 1.0, 0.0).astype(BF16)
        return jnp.dot(sel[...], z_ref[:, col:col + width], preferred_element_type=F32)

    exchange(produce, load_all(((z_hbm, z_ref), (place_hbm, place_ref)), load_sem), resid_hbm, out_ref, *rest)


def reduce_call(kernel, operands, depth, resid, collective_id, name, limit):
    rows, width = resid.shape
    piece = rows // lax.axis_size("tp")
    vmem = pl.BlockSpec(memory_space=pltpu.VMEM)
    return pl.pallas_call(
        kernel,
        in_specs=[pl.BlockSpec(memory_space=pltpu.HBM)] * len(operands) + [pl.BlockSpec(memory_space=pl.ANY)],
        out_specs=vmem,
        out_shape=jax.ShapeDtypeStruct((rows, width), BF16),
        scratch_shapes=[pltpu.VMEM(op.shape, op.dtype) for op in operands] + [
            pltpu.SemaphoreType.DMA((len(operands),)),
            pltpu.VMEM((4, piece, width), BF16),
            pltpu.VMEM((4, piece, width), BF16),
            pltpu.VMEM((4, piece, width), F32),
            pltpu.VMEM((3, piece, width), BF16),
            pltpu.VMEM((piece, width), BF16),
            pltpu.VMEM((2, piece, width), BF16),
            pltpu.VMEM((piece, width), BF16),
            pltpu.VMEM((piece, width), BF16),
            pltpu.VMEM((piece, depth), BF16),
            pltpu.SemaphoreType.DMA,
            pltpu.SemaphoreType.DMA((6, 2)),
            pltpu.SemaphoreType.DMA((24, 2)),
            pltpu.SemaphoreType.DMA((13, 2)),
        ],
        compiler_params=pltpu.CompilerParams(collective_id=collective_id, has_side_effects=True, vmem_limit_bytes=limit),
        name=name,
    )(*operands, resid)


def mlp_kernel(rows, x_hbm, gain_ref, router_ref, ids_ref, wg_hbm, wu_hbm, wd_hbm, z_hbm, place_ref, x_ref, wg, wu, wd, normed, act, stage, blank, rank_ref, gate_ref, count_ref, flag_ref, sem, z_sem, blank_sem, x_sem):
    tokens, width = x_hbm.shape
    local, _, ffn = wg.shape
    experts = router_ref.shape[0]

    x_copy = pltpu.make_async_copy(x_hbm, x_ref, x_sem)
    x_copy.start()

    def weight(e, i):
        src, dst = ((wg_hbm, wg), (wu_hbm, wu), (wd_hbm, wd))[i]
        return pltpu.make_async_copy(src.at[e], dst.at[e], sem.at[e, i])

    ids_row = [ids_ref[j:j + 1, :] for j in range(2)]
    first = lax.axis_index("tp") * local
    local_iota = first + lax.broadcasted_iota(jnp.int32, (8, tokens), 0)
    hit = [(ids_row[j] == local_iota) for j in range(2)]
    member = jnp.where(hit[0] | hit[1], 1.0, 0.0)
    counts = [jnp.sum(member[e:e + 1, :]).astype(jnp.int32) for e in range(local)]
    busiest, most = jnp.int32(0), counts[0]
    for e in range(1, local):
        busiest = jnp.where(counts[e] > most, e, busiest)
        most = jnp.maximum(counts[e], most)

    def nth(i):
        return jnp.where(i == 0, busiest, jnp.where(i - 1 < busiest, i - 1, i))

    flag_ref[0] = 0
    flag_ref[1] = 0
    flag_ref[2] = 0

    def fetch():
        issued = flag_ref[2]

        @pl.when(issued < 3 * local)
        def _():
            e = nth(issued // 3)
            for i in range(3):
                @pl.when(issued % 3 == i)
                def _():
                    weight(e, i).start()
            flag_ref[2] = issued + 1

    for _ in range(3):
        fetch()

    step = 128
    blank[...] = jnp.zeros_like(blank)
    x_copy.wait()
    for t in range(0, tokens, step):
        xf = x_ref[t:t + step, :].astype(F32)
        inv = lax.rsqrt(jnp.mean(xf * xf, axis=-1, keepdims=True) + NORM_EPS)
        normed[t:t + step, :] = (xf * inv * gain_ref[...]).astype(BF16)

    logits = lax.dot_general(router_ref[...], normed[...], (((1,), (1,)), ((), ())), preferred_element_type=F32)
    expert_iota = lax.broadcasted_iota(jnp.int32, (experts, tokens), 0)
    picked = [jnp.sum(jnp.where(expert_iota == ids_row[j], logits, 0.0), axis=0, keepdims=True) for j in range(2)]
    top = jnp.maximum(picked[0], picked[1])
    raised = [jnp.exp(p - top) for p in picked]
    gate = [r / (raised[0] + raised[1]) for r in raised]
    gate_ref[...] = jnp.where(hit[0], gate[0], 0.0) + jnp.where(hit[1], gate[1], 0.0)
    tri = jnp.where(lax.broadcasted_iota(jnp.int32, (step, step), 0) <= lax.broadcasted_iota(jnp.int32, (step, step), 1), 1.0, 0.0).astype(BF16)
    running = jnp.zeros((8, 1), F32)
    for t in range(0, tokens, step):
        piece = member[:, t:t + step]
        inside = jnp.dot(piece.astype(BF16), tri, preferred_element_type=F32)
        rank_ref[:, t:t + step] = jnp.where(piece > 0, inside + running - 1.0, -1.0)
        running = running + jnp.sum(piece, axis=1, keepdims=True)

    start = jnp.int32(0)
    place = [jnp.full((1, tokens), -1.0, F32) for _ in range(2)]
    for e in range(local):
        count = counts[e]
        count_ref[e, 0] = count
        count_ref[e, 1] = start
        offset = (start * rows).astype(F32)
        place = [jnp.where(hit[j][e:e + 1, :], rank_ref[e:e + 1, :] + offset, place[j]) for j in range(2)]
        start = start + (count + rows - 1) // rows
    for j in range(2):
        place_ref[j:j + 1, :] = place[j]

    def blank_copy(i):
        return pltpu.make_async_copy(blank, z_hbm.at[pl.ds(pl.multiple_of(i * rows, rows), rows)], blank_sem)

    def z_copy(i, slot, n):
        return pltpu.make_async_copy(stage.at[slot, pl.ds(0, n * rows)], z_hbm.at[pl.ds(pl.multiple_of(i * rows, rows), n * rows)], z_sem.at[slot])

    total_tiles = z_hbm.shape[0] // rows
    used = start

    def blank_start(i, carry):
        blank_copy(i).start()
        return carry

    def tile(e, base, n, z_row):
        size = n * rows
        hits = rank_ref[pl.ds(e, 1), :] == (lax.broadcasted_iota(jnp.int32, (size, tokens), 0) + base).astype(F32)
        gate_col = jnp.sum(jnp.where(hits, gate_ref[pl.ds(e, 1), :], 0.0), axis=1, keepdims=True)
        picked_rows = jnp.dot(jnp.where(hits, 1.0, 0.0).astype(BF16), normed[...], preferred_element_type=F32).astype(BF16)
        for f in range(0, ffn, 512):
            g = jnp.dot(picked_rows, wg[e, :, f:f + 512], preferred_element_type=F32)
            u = jnp.dot(picked_rows, wu[e, :, f:f + 512], preferred_element_type=F32)
            act[:size, f:f + 512] = (jax.nn.silu(g) * u).astype(BF16)

        fetch()

        @pl.when(base == 0)
        def _():
            weight(e, 2).wait()
            fetch()

        down = jnp.dot(act[:size, :], wd[e], preferred_element_type=F32) * gate_col
        slot = n - 1

        @pl.when(flag_ref[slot] == 1)
        def _():
            z_copy(0, slot, n).wait()

        stage[slot, :size, :] = down.astype(BF16)
        z_copy(z_row, slot, n).start()
        flag_ref[slot] = 1
        fetch()

    def expert_step(turn, carry):
        e = nth(turn)
        count = count_ref[e, 0]
        begin = count_ref[e, 1]
        weight(e, 0).wait()
        fetch()
        weight(e, 1).wait()
        fetch()
        pairs = (count + rows - 1) // (2 * rows)

        def pair_step(i, inner):
            tile(e, i * (2 * rows), 2, begin + 2 * i)
            return inner

        lax.fori_loop(0, pairs, pair_step, 0)

        @pl.when(count > pairs * (2 * rows))
        def _():
            tile(e, pairs * (2 * rows), 1, begin + 2 * pairs)

        @pl.when(count == 0)
        def _():
            weight(e, 2).wait()
            fetch()

        @pl.when(turn == 0)
        def _():
            lax.fori_loop(used, total_tiles, blank_start, 0)

        return carry

    lax.fori_loop(0, local, expert_step, 0)

    def blank_wait(i, carry):
        blank_copy(i).wait()
        return carry

    lax.fori_loop(used, total_tiles, blank_wait, 0)
    for slot in range(2):
        @pl.when(flag_ref[slot] == 1)
        def _():
            z_copy(0, slot, slot + 1).wait()


def experts_mlp(x1, mlp_ids, norm_mlp, router_mlp, w_gate, w_up, w_down, rows=128):
    tokens, width = x1.shape
    local, _, ffn = w_gate.shape
    vmem = pl.BlockSpec(memory_space=pltpu.VMEM)
    hbm = pl.BlockSpec(memory_space=pl.ANY)
    return pl.pallas_call(
        functools.partial(mlp_kernel, rows),
        in_specs=[hbm, vmem, vmem, vmem, hbm, hbm, hbm],
        out_specs=[hbm, vmem],
        out_shape=[jax.ShapeDtypeStruct((2 * tokens + local * rows, width), BF16), jax.ShapeDtypeStruct((2, tokens), F32)],
        scratch_shapes=[
            pltpu.VMEM((tokens, width), BF16),
            pltpu.VMEM((local, width, ffn), BF16),
            pltpu.VMEM((local, width, ffn), BF16),
            pltpu.VMEM((local, ffn, width), BF16),
            pltpu.VMEM((tokens, width), BF16),
            pltpu.VMEM((2 * rows, ffn), BF16),
            pltpu.VMEM((2, 2 * rows, width), BF16),
            pltpu.VMEM((rows, width), BF16),
            pltpu.VMEM((8, tokens), F32),
            pltpu.VMEM((8, tokens), F32),
            pltpu.SMEM((local, 2), jnp.int32),
            pltpu.SMEM((3,), jnp.int32),
            pltpu.SemaphoreType.DMA((local, 3)),
            pltpu.SemaphoreType.DMA((2,)),
            pltpu.SemaphoreType.DMA,
            pltpu.SemaphoreType.DMA,
        ],
        compiler_params=pltpu.CompilerParams(vmem_limit_bytes=VMEM_LIMIT),
        name="experts",
    )(x1, norm_mlp.reshape(1, width), router_mlp.T, mlp_ids.T, w_gate, w_up, w_down)


def solution(mesh):
    def local_step(x, k_cache, v_cache, positions, att_ids, mlp_ids, norm_att, w_kv, router_att, w_query, w_out, norm_mlp, router_mlp, w_gate, w_up, w_down):
        o, gate, keys_all, values_all = attention(x, k_cache, v_cache, positions, att_ids, norm_att, w_kv, router_att, w_query)
        depth = w_out.shape[0] * w_out.shape[1]
        x_mid = reduce_call(project_kernel, (o, att_ids.T, gate, w_out.reshape(depth, x.shape[1])), depth, x, 0, "project", VMEM_LIMIT)
        z, place = experts_mlp(x_mid, mlp_ids, norm_mlp, router_mlp, w_gate, w_up, w_down)
        x_out = reduce_call(combine_kernel, (z, place), z.shape[0], x_mid, 1, "combine", 50 * 1024 * 1024)
        return x_out, keys_all, values_all

    token_spec = P('dp', None)
    cache_spec = P('dp', None, 'tp', None)
    expert_spec = P('tp', None, None)
    in_specs = (token_spec, cache_spec, cache_spec, P('dp'), token_spec, token_spec, P(), P(None, 'tp', None), P(), P(None, None, 'tp'), P(None, 'tp', None), P(), P(), expert_spec, expert_spec, expert_spec)
    out_specs = (token_spec, cache_spec, cache_spec)
    return jax.shard_map(local_step, mesh=mesh, in_specs=in_specs, out_specs=out_specs, check_vma=False)
```

```python
import functools

import jax
import jax.numpy as jnp
import numpy as np
from jax import lax
from jax.experimental import pallas as pl
from jax.experimental.pallas import tpu as pltpu
from jax.sharding import PartitionSpec as P

NORM_EPS = 1e-6
ROPE_BASE = 10000.0
F32 = jnp.float32
BF16 = jnp.bfloat16
VMEM_LIMIT = 67043328
MESH = pl.DeviceIdType.MESH


NEG = -1e30


def attn_kernel(x_ref, gain_ref, wkv_ref, router_ref, wq_ref, pos_ref, ids_ref, freq_ref, k_ref, v_ref, o_ref, gate_ref, ko_ref, vo_ref, sc_ref, fold_ref, kv_ref):
    block, width = x_ref.shape
    slots, heads, dim, _ = k_ref.shape
    experts = wq_ref.shape[0]
    cols = heads * dim
    half = dim // 2
    xf = x_ref[...].astype(F32)
    inv = lax.rsqrt(jnp.mean(xf * xf, axis=-1, keepdims=True) + NORM_EPS)
    hidden = (xf * inv * gain_ref[...]).astype(BF16)
    pos = pos_ref[...]
    angles = freq_ref[...] * pos.astype(F32)
    cos_t = jnp.cos(angles)
    sin_t = jnp.sin(angles)

    @pl.when(pl.program_id(0) == 0)
    def _():
        for n in range(heads):
            kv_ref[:, n * 2 * dim:(n + 1) * 2 * dim] = wkv_ref[:, n, :]

    def rope(head):
        first, second = head[:half], head[half:]
        return jnp.concatenate([first * cos_t - second * sin_t, second * cos_t + first * sin_t], axis=0)

    kv_t = jnp.dot(hidden, kv_ref[...], preferred_element_type=F32).T
    k_new = [rope(kv_t[n * 2 * dim:n * 2 * dim + dim]).astype(BF16) for n in range(heads)]
    v_new = [kv_t[n * 2 * dim + dim:(n + 1) * 2 * dim].astype(BF16) for n in range(heads)]

    logits = lax.dot_general(router_ref[...], hidden, (((1,), (1,)), ((), ())), preferred_element_type=F32)
    ids_row = [ids_ref[j:j + 1, :] for j in range(2)]
    expert_iota = lax.broadcasted_iota(jnp.int32, (experts, block), 0)
    picked = [jnp.sum(jnp.where(expert_iota == ids_row[j], logits, 0.0), axis=0, keepdims=True) for j in range(2)]
    top = jnp.maximum(picked[0], picked[1])
    raised = [jnp.exp(p - top) for p in picked]
    gate = [r / (raised[0] + raised[1]) for r in raised]
    ids_col = [jnp.broadcast_to(ids_row[j], (cols, block)).T for j in range(2)]
    for j in range(2):
        gate_ref[j:j + 1, :] = gate[j]

    chosen = [jnp.zeros((block, cols), F32) for _ in range(2)]
    for e in range(0, experts, 2):
        q_two = jnp.dot(hidden, jnp.concatenate([wq_ref[e], wq_ref[e + 1]], axis=1), preferred_element_type=F32)
        for i in range(2):
            q_e = q_two[:, i * cols:(i + 1) * cols]
            chosen = [jnp.where(ids_col[j] == e + i, q_e, chosen[j]) for j in range(2)]
    q_rot = []
    for j in range(2):
        q_t = chosen[j].T
        q_rot.append([rope(q_t[n * dim:(n + 1) * dim]).astype(BF16).astype(F32) for n in range(heads)])

    pos16 = jnp.broadcast_to(pos.astype(F32), (dim, block)).astype(BF16)

    def score_step(s, carry):
        at_slot = pos16 == jnp.full((dim, block), s, jnp.int32).astype(F32).astype(BF16)
        for n in range(heads):
            packed = k_ref[s, n]
            keys = packed.astype(F32)
            for j in range(2):
                fold_ref[j * heads + n, pl.ds(pl.multiple_of(s * 8, 8), 8), :] = jnp.sum((q_rot[j][n] * keys).reshape(dim // 8, 8, block), axis=0)
            ko_ref[s, n] = jnp.where(at_slot, k_new[n], packed)
        return carry

    lax.fori_loop(0, slots, score_step, 0, unroll=4)

    slot_iota = lax.broadcasted_iota(jnp.int32, (slots, block), 0)
    here = slot_iota == pos
    visible = slot_iota <= pos
    out = []
    for j in range(2):
        for n in range(heads):
            fresh = jnp.sum(q_rot[j][n] * k_new[n].astype(F32), axis=0, keepdims=True)
            score = fold_ref[j * heads + n, pl.ds(0, slots, stride=8), :]
            for r in range(1, 8):
                score = score + fold_ref[j * heads + n, pl.ds(r, slots, stride=8), :]
            score = jnp.where(here, fresh, score) * dim ** -0.5
            score = jnp.where(visible, score, NEG)
            raised_s = jnp.exp(score - jnp.max(score, axis=0, keepdims=True))
            prob = (raised_s / jnp.sum(raised_s, axis=0, keepdims=True)).astype(BF16).astype(F32)
            own = jnp.sum(jnp.where(here, prob, 0.0), axis=0, keepdims=True)
            sc_ref[j * heads + n] = jnp.where(here, 0.0, prob)
            out.append(own * v_new[n].astype(F32))

    def value_step(s, carry):
        at_slot = pos16 == jnp.full((dim, block), s, jnp.int32).astype(F32).astype(BF16)
        carry = list(carry)
        for n in range(heads):
            packed = v_ref[s, n]
            values = packed.astype(F32)
            for j in range(2):
                i = j * heads + n
                carry[i] = carry[i] + sc_ref[i, pl.ds(s, 1), :] * values
            vo_ref[s, n] = jnp.where(at_slot, v_new[n], packed)
        return tuple(carry)

    out = lax.fori_loop(0, slots, value_step, tuple(out), unroll=4)

    for j in range(2):
        o_ref[j] = jnp.concatenate(out[j * heads:(j + 1) * heads], axis=0).T.astype(BF16)


def attention(x, k_cache, v_cache, positions, att_ids, norm_att, w_kv, router_att, w_query, block=128):
    tokens, width = x.shape
    _, slots, heads, dim = k_cache.shape
    experts = w_query.shape[0]
    cols = heads * dim
    half = dim // 2
    inv_freq = jnp.asarray(ROPE_BASE ** (-(np.arange(half) * 2.0 / dim)), F32)
    k_t = k_cache.transpose(1, 2, 3, 0)
    v_t = v_cache.transpose(1, 2, 3, 0)
    whole = lambda *shape: pl.BlockSpec(shape, lambda i: (0,) * len(shape), pipeline_mode=pl.Buffered(1))
    lane = lambda rows: pl.BlockSpec((rows, block), lambda i: (0, i))
    cache = pl.BlockSpec((slots, heads, dim, block), lambda i: (0, 0, 0, i))
    row = pl.BlockSpec((block, width), lambda i: (i, 0))
    o, gate, k_out, v_out = pl.pallas_call(
        attn_kernel,
        grid=(tokens // block,),
        in_specs=[row, whole(1, width), whole(width, heads, 2 * dim), whole(experts, width), whole(experts, width, cols), lane(1), lane(2), whole(half, 1), cache, cache],
        out_specs=[pl.BlockSpec((2, block, cols), lambda i: (0, i, 0)), lane(2), cache, cache],
        out_shape=[jax.ShapeDtypeStruct((2, tokens, cols), BF16), jax.ShapeDtypeStruct((2, tokens), F32), jax.ShapeDtypeStruct(k_t.shape, BF16), jax.ShapeDtypeStruct(v_t.shape, BF16)],
        scratch_shapes=[pltpu.VMEM((2 * heads, slots, block), F32), pltpu.VMEM((2 * heads, slots * 8, block), F32), pltpu.VMEM((width, 2 * cols), BF16)],
        compiler_params=pltpu.CompilerParams(dimension_semantics=("arbitrary",), vmem_limit_bytes=VMEM_LIMIT),
        name="attention",
    )(x, norm_att.reshape(1, width), w_kv, router_att.T, w_query, positions.reshape(1, tokens), att_ids.T, inv_freq[:, None], k_t, v_t)
    return o, gate, k_out.transpose(3, 0, 1, 2), v_out.transpose(3, 0, 1, 2)


def exchange(cuts, produce, loads, carried, resid_hbm, out_ref, stage, pair_in, held, ring, far_in, full_in, own, resid, sel, resid_sem, swap_sem, ring_sem, d2d_sem):
    rows, width = out_ref.shape
    mine = rows // 2
    chips = lax.axis_size("tp") // 2
    piece = mine // chips
    cw = piece // cuts
    near = cuts // 2
    order = [k for pair in zip(range(near), range(near, cuts)) for k in pair]
    me = lax.axis_index("tp")
    core = lax.rem(me, 2)
    chip = me // 2
    other = 1 - core
    right_chip = lax.rem(chip + 1, chips)
    left_chip = lax.rem(chip + chips - 1, chips)
    far_chip = lax.rem(chip + 2, chips)
    partner = {"tp": chip * 2 + other}
    right = {"tp": right_chip * 2 + core}
    left = {"tp": left_chip * 2 + core}

    barrier = pltpu.get_barrier_semaphore()
    for peer in (partner, right, left):
        pl.semaphore_signal(barrier, inc=1, device_id=peer, device_id_type=MESH)
    for copy in loads:
        copy.start()

    def first_row(c, q):
        return pl.multiple_of(c * mine + q * piece, piece)

    def rows_of(c, q):
        return pl.ds(first_row(c, q), piece)

    resid_copy = pltpu.make_async_copy(resid_hbm.at[rows_of(core, chip)], resid, resid_sem)
    resid_copy.start()
    for copy in loads:
        copy.wait()
    for copy in carried:
        copy.start()
    pending = []

    def send(src, dst, sem, peer):
        copy = pltpu.make_async_remote_copy(src_ref=src, dst_ref=dst, send_sem=sem.at[0], recv_sem=sem.at[1], device_id=peer, device_id_type=MESH)
        copy.start()
        pending.append(copy)
        return copy

    def cut(k):
        return slice(k * cw, (k + 1) * cw)

    def dcut(k):
        return pl.ds(k * cw, cw)

    def swap(slot, q):
        stage[slot] = produce(first_row(other, q), 0, width, sel).astype(BF16)
        if slot == 0:
            pl.semaphore_wait(barrier, 3)
        copy = send(stage.at[slot], pair_in.at[slot], swap_sem.at[slot], partner)
        held[slot] = produce(first_row(core, q), 0, width, sel)
        return copy

    def land(copy, slot):
        copy.wait_recv()
        held[slot] += pair_in[slot].astype(F32)

    far, plain, added = {}, {}, {}
    land(swap(0, far_chip), 0)
    ring[0] = held[0].astype(BF16)
    for k in order:
        far[k] = send(ring.at[0, dcut(k)], far_in.at[dcut(k)], ring_sem.at[k], right if k < near else left)
    land(swap(1, right_chip), 1)
    ring[1, near * cw:] = held[1, near * cw:].astype(BF16)
    for k in range(near, cuts):
        plain[k] = send(ring.at[1, dcut(k)], full_in.at[0, dcut(k)], ring_sem.at[cuts + k], right)
    land(swap(2, left_chip), 2)
    ring[2, :near * cw] = held[2, :near * cw].astype(BF16)
    for k in range(near):
        plain[k] = send(ring.at[2, dcut(k)], full_in.at[1, dcut(k)], ring_sem.at[cuts + k], left)
    for k in order:
        slot = 1 if k < near else 2
        far[k].wait_recv()
        ring[slot, cut(k)] = (held[slot, cut(k)] + far_in[cut(k)].astype(F32)).astype(BF16)
        added[k] = send(ring.at[slot, dcut(k)], full_in.at[slot - 1, dcut(k)], ring_sem.at[2 * cuts + k], right if k < near else left)
    land(swap(3, chip), 3)
    resid_copy.wait()

    own_rows, left_rows, right_rows, far_rows = (rows_of(core, q) for q in (chip, left_chip, right_chip, far_chip))
    to_right, to_left = {}, {}

    def inside(rows_start, k):
        return pl.ds(pl.multiple_of(rows_start + k * cw, cw), cw)

    own_row, left_row, right_row, far_row = (first_row(core, q) for q in (chip, left_chip, right_chip, far_chip))
    for k in order:
        plain[k].wait_recv()
        added[k].wait_recv()
        own[cut(k), :] = (resid[cut(k), :].astype(F32) + (held[3, cut(k), :] + full_in[0, cut(k), :].astype(F32) + full_in[1, cut(k), :].astype(F32))).astype(BF16)
        first, second = ((right, to_right, 3), (left, to_left, 4))[::1 if k < near else -1]
        for peer, table, base in (first, second):
            table[k] = send(own.at[dcut(k)], out_ref.at[inside(own_row, k)], ring_sem.at[base * cuts + k], peer)
    d2d = [send(own, out_ref.at[own_rows], d2d_sem.at[0], partner)]
    out_ref[own_rows, :] = own[...]
    onward = {}
    for k in order:
        if k < near:
            to_right[k].wait_recv()
            onward[k] = send(out_ref.at[inside(left_row, k)], out_ref.at[inside(left_row, k)], ring_sem.at[5 * cuts + k], right)
        else:
            to_left[k].wait_recv()
            onward[k] = send(out_ref.at[inside(right_row, k)], out_ref.at[inside(right_row, k)], ring_sem.at[5 * cuts + k], left)
    for k in range(near, cuts):
        to_right[k].wait_recv()
    d2d.append(send(out_ref.at[left_rows], out_ref.at[left_rows], d2d_sem.at[1], partner))
    for k in range(near):
        to_left[k].wait_recv()
    d2d.append(send(out_ref.at[right_rows], out_ref.at[right_rows], d2d_sem.at[2], partner))
    for i, k in enumerate(order):
        onward[k].wait_recv()
        d2d.append(send(out_ref.at[inside(far_row, k)], out_ref.at[inside(far_row, k)], d2d_sem.at[3 + i], partner))
    for copy in carried:
        copy.wait()
    for copy in d2d:
        copy.wait_recv()
    for copy in pending:
        copy.wait_send()


def load_all(pairs, sem):
    return [pltpu.make_async_copy(src, dst, sem.at[i]) for i, (src, dst) in enumerate(pairs)]


def project_kernel(o_hbm, ids_hbm, gate_hbm, wo_hbm, wg_hbm, wu_hbm, resid_hbm, out_ref, wg_ref, wu_ref, o_ref, ids_ref, gate_ref, wo_ref, load_sem, carry_sem, *rest):
    cols = o_ref.shape[2]
    experts = wo_ref.shape[0] // cols

    def produce(start, col, width, sel):
        block = sel.shape[0]
        total = None
        for j in range(2):
            ids_col = jnp.broadcast_to(ids_ref[j:j + 1, pl.ds(start, block)], (cols, block)).T
            gate_col = jnp.broadcast_to(gate_ref[j:j + 1, pl.ds(start, block)], (cols, block)).T
            o_j = o_ref[j, pl.ds(start, block), :].astype(F32)
            for e in range(experts):
                sel[:, e * cols:(e + 1) * cols] = jnp.where(ids_col == e, o_j, 0.0).astype(BF16)
            projected = jnp.dot(sel[...], wo_ref[:, col:col + width], preferred_element_type=F32)
            scaled = projected * jnp.concatenate([gate_col] * (width // cols), axis=1)
            total = scaled if total is None else total + scaled
        return total

    exchange(4, produce, load_all(((o_hbm, o_ref), (ids_hbm, ids_ref), (gate_hbm, gate_ref), (wo_hbm, wo_ref)), load_sem), load_all(((wg_hbm, wg_ref), (wu_hbm, wu_ref)), carry_sem), resid_hbm, out_ref, *rest)


def combine_kernel(z_hbm, place_hbm, resid_hbm, out_ref, z_ref, place_ref, load_sem, carry_sem, *rest):
    def produce(start, col, width, sel):
        block = sel.shape[0]
        place = [jnp.broadcast_to(place_ref[j:j + 1, pl.ds(start, block)], (block, block)).T for j in range(2)]
        lane = lax.broadcasted_iota(jnp.int32, (block, block), 1).astype(F32)
        for r in range(0, sel.shape[1], block):
            here = lane + float(r)
            sel[:, r:r + block] = jnp.where((place[0] == here) | (place[1] == here), 1.0, 0.0).astype(BF16)
        return jnp.dot(sel[...], z_ref[:, col:col + width], preferred_element_type=F32)

    exchange(4, produce, load_all(((z_hbm, z_ref), (place_hbm, place_ref)), load_sem), [], resid_hbm, out_ref, *rest)


def reduce_call(kernel, operands, depth, resid, collective_id, name, limit, carried=()):
    rows, width = resid.shape
    piece = rows // lax.axis_size("tp")
    vmem = pl.BlockSpec(memory_space=pltpu.VMEM)
    return pl.pallas_call(
        kernel,
        in_specs=[pl.BlockSpec(memory_space=pltpu.HBM)] * (len(operands) + len(carried)) + [pl.BlockSpec(memory_space=pl.ANY)],
        out_specs=[vmem] * (1 + len(carried)),
        out_shape=[jax.ShapeDtypeStruct(resid.shape, BF16)] + [pltpu.VMEM(a.shape, a.dtype) for a in carried],
        scratch_shapes=[pltpu.VMEM(op.shape, op.dtype) for op in operands] + [
            pltpu.SemaphoreType.DMA((len(operands),)),
            pltpu.SemaphoreType.DMA((2,)),
            pltpu.VMEM((4, piece, width), BF16),
            pltpu.VMEM((4, piece, width), BF16),
            pltpu.VMEM((4, piece, width), F32),
            pltpu.VMEM((3, piece, width), BF16),
            pltpu.VMEM((piece, width), BF16),
            pltpu.VMEM((2, piece, width), BF16),
            pltpu.VMEM((piece, width), BF16),
            pltpu.VMEM((piece, width), BF16),
            pltpu.VMEM((piece, depth), BF16),
            pltpu.SemaphoreType.DMA,
            pltpu.SemaphoreType.DMA((4, 2)),
            pltpu.SemaphoreType.DMA((24, 2)),
            pltpu.SemaphoreType.DMA((13, 2)),
        ],
        compiler_params=pltpu.CompilerParams(collective_id=collective_id, has_side_effects=True, vmem_limit_bytes=limit),
        name=name,
    )(*operands, *carried, resid)


def mlp_kernel(rows, x_hbm, gain_ref, router_ref, ids_ref, wg, wu, wd_hbm, z_hbm, place_ref, x_ref, wd, normed, act, stage, blank, rank_ref, gate_ref, count_ref, flag_ref, sem, z_sem, blank_sem, x_sem):
    tokens, width = x_hbm.shape
    local, _, ffn = wg.shape
    experts = router_ref.shape[0]

    x_copy = pltpu.make_async_copy(x_hbm, x_ref, x_sem)
    x_copy.start()

    def weight(e):
        return pltpu.make_async_copy(wd_hbm.at[e], wd.at[e], sem.at[e])

    ids_row = [ids_ref[j:j + 1, :] for j in range(2)]
    first = lax.axis_index("tp") * local
    local_iota = first + lax.broadcasted_iota(jnp.int32, (8, tokens), 0)
    hit = [(ids_row[j] == local_iota) for j in range(2)]
    member = jnp.where(hit[0] | hit[1], 1.0, 0.0)
    counts = [jnp.sum(member[e:e + 1, :]).astype(jnp.int32) for e in range(local)]
    busiest, most = jnp.int32(0), counts[0]
    for e in range(1, local):
        busiest = jnp.where(counts[e] > most, e, busiest)
        most = jnp.maximum(counts[e], most)

    def nth(i):
        return jnp.where(i == 0, busiest, jnp.where(i - 1 < busiest, i - 1, i))

    flag_ref[0] = 0
    flag_ref[1] = 0
    flag_ref[2] = 0

    def fetch():
        issued = flag_ref[2]

        @pl.when(issued < local)
        def _():
            weight(nth(issued)).start()
            flag_ref[2] = issued + 1

    for _ in range(2):
        fetch()

    step = 128
    blank[...] = jnp.zeros_like(blank)
    x_copy.wait()
    for t in range(0, tokens, step):
        xf = x_ref[t:t + step, :].astype(F32)
        inv = lax.rsqrt(jnp.mean(xf * xf, axis=-1, keepdims=True) + NORM_EPS)
        normed[t:t + step, :] = (xf * inv * gain_ref[...]).astype(BF16)

    logits = lax.dot_general(router_ref[...], normed[...], (((1,), (1,)), ((), ())), preferred_element_type=F32)
    expert_iota = lax.broadcasted_iota(jnp.int32, (experts, tokens), 0)
    picked = [jnp.sum(jnp.where(expert_iota == ids_row[j], logits, 0.0), axis=0, keepdims=True) for j in range(2)]
    top = jnp.maximum(picked[0], picked[1])
    raised = [jnp.exp(p - top) for p in picked]
    gate = [r / (raised[0] + raised[1]) for r in raised]
    gate_ref[...] = jnp.where(hit[0], gate[0], 0.0) + jnp.where(hit[1], gate[1], 0.0)
    tri = jnp.where(lax.broadcasted_iota(jnp.int32, (step, step), 0) <= lax.broadcasted_iota(jnp.int32, (step, step), 1), 1.0, 0.0).astype(BF16)
    running = jnp.zeros((8, 1), F32)
    for t in range(0, tokens, step):
        piece = member[:, t:t + step]
        inside = jnp.dot(piece.astype(BF16), tri, preferred_element_type=F32)
        rank_ref[:, t:t + step] = jnp.where(piece > 0, inside + running - 1.0, -1.0)
        running = running + jnp.sum(piece, axis=1, keepdims=True)

    start = jnp.int32(0)
    place = [jnp.full((1, tokens), -1.0, F32) for _ in range(2)]
    for e in range(local):
        count = counts[e]
        count_ref[e, 0] = count
        count_ref[e, 1] = start
        offset = (start * rows).astype(F32)
        place = [jnp.where(hit[j][e:e + 1, :], rank_ref[e:e + 1, :] + offset, place[j]) for j in range(2)]
        start = start + (count + rows - 1) // rows
    for j in range(2):
        place_ref[j:j + 1, :] = place[j]

    def blank_copy(i):
        return pltpu.make_async_copy(blank, z_hbm.at[pl.ds(pl.multiple_of(i * rows, rows), rows)], blank_sem)

    def z_copy(i, slot, n):
        return pltpu.make_async_copy(stage.at[slot, pl.ds(0, n * rows)], z_hbm.at[pl.ds(pl.multiple_of(i * rows, rows), n * rows)], z_sem.at[slot])

    total_tiles = z_hbm.shape[0] // rows
    used = start

    def blank_start(i, carry):
        blank_copy(i).start()
        return carry

    def tile(e, base, n, z_row):
        size = n * rows
        hits = rank_ref[pl.ds(e, 1), :] == (lax.broadcasted_iota(jnp.int32, (size, tokens), 0) + base).astype(F32)
        gate_col = jnp.sum(jnp.where(hits, gate_ref[pl.ds(e, 1), :], 0.0), axis=1, keepdims=True)
        picked_rows = jnp.dot(jnp.where(hits, 1.0, 0.0).astype(BF16), normed[...], preferred_element_type=F32).astype(BF16)
        for f in range(0, ffn, 512):
            g = jnp.dot(picked_rows, wg[e, :, f:f + 512], preferred_element_type=F32)
            u = jnp.dot(picked_rows, wu[e, :, f:f + 512], preferred_element_type=F32)
            act[:size, f:f + 512] = (jax.nn.silu(g) * u).astype(BF16)

        fetch()

        @pl.when(base == 0)
        def _():
            weight(e).wait()
            fetch()

        down = jnp.dot(act[:size, :], wd[e], preferred_element_type=F32) * gate_col
        slot = n - 1

        @pl.when(flag_ref[slot] == 1)
        def _():
            z_copy(0, slot, n).wait()

        stage[slot, :size, :] = down.astype(BF16)
        z_copy(z_row, slot, n).start()
        flag_ref[slot] = 1
        fetch()

    def expert_step(turn, carry):
        e = nth(turn)
        count = count_ref[e, 0]
        begin = count_ref[e, 1]
        pairs = (count + rows - 1) // (2 * rows)

        def pair_step(i, inner):
            tile(e, i * (2 * rows), 2, begin + 2 * i)
            return inner

        lax.fori_loop(0, pairs, pair_step, 0)

        @pl.when(count > pairs * (2 * rows))
        def _():
            tile(e, pairs * (2 * rows), 1, begin + 2 * pairs)

        @pl.when(count == 0)
        def _():
            weight(e).wait()
            fetch()

        @pl.when(turn == 0)
        def _():
            lax.fori_loop(used, total_tiles, blank_start, 0)

        return carry

    lax.fori_loop(0, local, expert_step, 0)

    def blank_wait(i, carry):
        blank_copy(i).wait()
        return carry

    lax.fori_loop(used, total_tiles, blank_wait, 0)
    for slot in range(2):
        @pl.when(flag_ref[slot] == 1)
        def _():
            z_copy(0, slot, slot + 1).wait()


def experts_mlp(x1, mlp_ids, norm_mlp, router_mlp, w_gate, w_up, w_down, rows=128):
    tokens, width = x1.shape
    local, _, ffn = w_gate.shape
    vmem = pl.BlockSpec(memory_space=pltpu.VMEM)
    hbm = pl.BlockSpec(memory_space=pl.ANY)
    return pl.pallas_call(
        functools.partial(mlp_kernel, rows),
        in_specs=[hbm, vmem, vmem, vmem, vmem, vmem, hbm],
        out_specs=[hbm, vmem],
        out_shape=[jax.ShapeDtypeStruct((2 * tokens + local * rows, width), BF16), jax.ShapeDtypeStruct((2, tokens), F32)],
        scratch_shapes=[
            pltpu.VMEM((tokens, width), BF16),
            pltpu.VMEM((local, ffn, width), BF16),
            pltpu.VMEM((tokens, width), BF16),
            pltpu.VMEM((2 * rows, ffn), BF16),
            pltpu.VMEM((2, 2 * rows, width), BF16),
            pltpu.VMEM((rows, width), BF16),
            pltpu.VMEM((8, tokens), F32),
            pltpu.VMEM((8, tokens), F32),
            pltpu.SMEM((local, 2), jnp.int32),
            pltpu.SMEM((3,), jnp.int32),
            pltpu.SemaphoreType.DMA((local,)),
            pltpu.SemaphoreType.DMA((2,)),
            pltpu.SemaphoreType.DMA,
            pltpu.SemaphoreType.DMA,
        ],
        compiler_params=pltpu.CompilerParams(vmem_limit_bytes=27 * 1024 * 1024),
        name="experts",
    )(x1, norm_mlp.reshape(1, width), router_mlp.T, mlp_ids.T, pltpu.with_memory_space_constraint(w_gate, pltpu.VMEM), pltpu.with_memory_space_constraint(w_up, pltpu.VMEM), w_down)


def solution(mesh):
    def local_step(x, k_cache, v_cache, positions, att_ids, mlp_ids, norm_att, w_kv, router_att, w_query, w_out, norm_mlp, router_mlp, w_gate, w_up, w_down):
        o, gate, keys_all, values_all = attention(x, k_cache, v_cache, positions, att_ids, norm_att, w_kv, router_att, w_query)
        depth = w_out.shape[0] * w_out.shape[1]
        x_mid, w_gate, w_up = reduce_call(project_kernel, (o, att_ids.T, gate, w_out.reshape(depth, x.shape[1])), depth, x, 0, "project", 27 * 1024 * 1024, (w_gate, w_up))
        z, place = experts_mlp(x_mid, mlp_ids, norm_mlp, router_mlp, w_gate, w_up, w_down)
        x_out, = reduce_call(combine_kernel, (z, place), z.shape[0], x_mid, 1, "combine", 50 * 1024 * 1024)
        return x_out, keys_all, values_all

    token_spec = P('dp', None)
    cache_spec = P('dp', None, 'tp', None)
    expert_spec = P('tp', None, None)
    in_specs = (token_spec, cache_spec, cache_spec, P('dp'), token_spec, token_spec, P(), P(None, 'tp', None), P(), P(None, None, 'tp'), P(None, 'tp', None), P(), P(), expert_spec, expert_spec, expert_spec)
    out_specs = (token_spec, cache_spec, cache_spec)
    return jax.shard_map(local_step, mesh=mesh, in_specs=in_specs, out_specs=out_specs, check_vma=False)
```

```python
import functools

import jax
import jax.numpy as jnp
import numpy as np
from jax import lax
from jax.experimental import pallas as pl
from jax.experimental.pallas import tpu as pltpu
from jax.sharding import PartitionSpec as P

NORM_EPS = 1e-6
ROPE_BASE = 10000.0
F32 = jnp.float32
BF16 = jnp.bfloat16
VMEM_LIMIT = 67043328
MESH = pl.DeviceIdType.MESH


NEG = -1e30


def attn_kernel(x_ref, gain_ref, wkv_ref, router_ref, wq_ref, pos_ref, ids_ref, freq_ref, k_ref, v_ref, o_ref, gate_ref, ko_ref, vo_ref, sc_ref, fold_ref, kv_ref):
    block, width = x_ref.shape
    slots, heads, dim, _ = k_ref.shape
    experts = wq_ref.shape[0]
    cols = heads * dim
    half = dim // 2
    xf = x_ref[...].astype(F32)
    inv = lax.rsqrt(jnp.mean(xf * xf, axis=-1, keepdims=True) + NORM_EPS)
    hidden = (xf * inv * gain_ref[...]).astype(BF16)
    pos = pos_ref[...]
    angles = freq_ref[...] * pos.astype(F32)
    cos_t = jnp.cos(angles)
    sin_t = jnp.sin(angles)

    @pl.when(pl.program_id(0) == 0)
    def _():
        for n in range(heads):
            kv_ref[:, n * 2 * dim:(n + 1) * 2 * dim] = wkv_ref[:, n, :]

    def rope(head):
        first, second = head[:half], head[half:]
        return jnp.concatenate([first * cos_t - second * sin_t, second * cos_t + first * sin_t], axis=0)

    kv_t = jnp.dot(hidden, kv_ref[...], preferred_element_type=F32).T
    k_new = [rope(kv_t[n * 2 * dim:n * 2 * dim + dim]).astype(BF16) for n in range(heads)]
    v_new = [kv_t[n * 2 * dim + dim:(n + 1) * 2 * dim].astype(BF16) for n in range(heads)]

    logits = lax.dot_general(router_ref[...], hidden, (((1,), (1,)), ((), ())), preferred_element_type=F32)
    ids_row = [ids_ref[j:j + 1, :] for j in range(2)]
    expert_iota = lax.broadcasted_iota(jnp.int32, (experts, block), 0)
    picked = [jnp.sum(jnp.where(expert_iota == ids_row[j], logits, 0.0), axis=0, keepdims=True) for j in range(2)]
    top = jnp.maximum(picked[0], picked[1])
    raised = [jnp.exp(p - top) for p in picked]
    gate = [r / (raised[0] + raised[1]) for r in raised]
    ids_col = [jnp.broadcast_to(ids_row[j], (cols, block)).T for j in range(2)]
    for j in range(2):
        gate_ref[j:j + 1, :] = gate[j]

    chosen = [jnp.zeros((block, cols), F32) for _ in range(2)]
    for e in range(0, experts, 2):
        q_two = jnp.dot(hidden, jnp.concatenate([wq_ref[e], wq_ref[e + 1]], axis=1), preferred_element_type=F32)
        for i in range(2):
            q_e = q_two[:, i * cols:(i + 1) * cols]
            chosen = [jnp.where(ids_col[j] == e + i, q_e, chosen[j]) for j in range(2)]
    q_rot = []
    for j in range(2):
        q_t = chosen[j].T
        q_rot.append([rope(q_t[n * dim:(n + 1) * dim]).astype(BF16).astype(F32) for n in range(heads)])

    pos16 = jnp.broadcast_to(pos.astype(F32), (dim, block)).astype(BF16)

    def score_step(s, carry):
        at_slot = pos16 == jnp.full((dim, block), s, jnp.int32).astype(F32).astype(BF16)
        for n in range(heads):
            packed = k_ref[s, n]
            keys = packed.astype(F32)
            for j in range(2):
                fold_ref[j * heads + n, pl.ds(pl.multiple_of(s * 8, 8), 8), :] = jnp.sum((q_rot[j][n] * keys).reshape(dim // 8, 8, block), axis=0)
            ko_ref[s, n] = jnp.where(at_slot, k_new[n], packed)
        return carry

    lax.fori_loop(0, slots, score_step, 0, unroll=16)

    slot_iota = lax.broadcasted_iota(jnp.int32, (slots, block), 0)
    here = slot_iota == pos
    visible = slot_iota <= pos
    out = []
    for j in range(2):
        for n in range(heads):
            fresh = jnp.sum(q_rot[j][n] * k_new[n].astype(F32), axis=0, keepdims=True)
            score = fold_ref[j * heads + n, pl.ds(0, slots, stride=8), :]
            for r in range(1, 8):
                score = score + fold_ref[j * heads + n, pl.ds(r, slots, stride=8), :]
            score = jnp.where(here, fresh, score) * dim ** -0.5
            score = jnp.where(visible, score, NEG)
            raised_s = jnp.exp(score - jnp.max(score, axis=0, keepdims=True))
            prob = (raised_s / jnp.sum(raised_s, axis=0, keepdims=True)).astype(BF16).astype(F32)
            own = jnp.sum(jnp.where(here, prob, 0.0), axis=0, keepdims=True)
            sc_ref[j * heads + n] = jnp.where(here, 0.0, prob)
            out.append(own * v_new[n].astype(F32))

    def value_step(s, carry):
        at_slot = pos16 == jnp.full((dim, block), s, jnp.int32).astype(F32).astype(BF16)
        carry = list(carry)
        for n in range(heads):
            packed = v_ref[s, n]
            values = packed.astype(F32)
            for j in range(2):
                i = j * heads + n
                carry[i] = carry[i] + sc_ref[i, pl.ds(s, 1), :] * values
            vo_ref[s, n] = jnp.where(at_slot, v_new[n], packed)
        return tuple(carry)

    out = lax.fori_loop(0, slots, value_step, tuple(out), unroll=16)

    for j in range(2):
        o_ref[j] = jnp.concatenate(out[j * heads:(j + 1) * heads], axis=0).T.astype(BF16)


def attention(x, k_cache, v_cache, positions, att_ids, norm_att, w_kv, router_att, w_query, block=128):
    tokens, width = x.shape
    _, slots, heads, dim = k_cache.shape
    experts = w_query.shape[0]
    cols = heads * dim
    half = dim // 2
    inv_freq = jnp.asarray(ROPE_BASE ** (-(np.arange(half) * 2.0 / dim)), F32)
    k_t = k_cache.transpose(1, 2, 3, 0)
    v_t = v_cache.transpose(1, 2, 3, 0)
    whole = lambda *shape: pl.BlockSpec(shape, lambda i: (0,) * len(shape), pipeline_mode=pl.Buffered(1))
    lane = lambda rows: pl.BlockSpec((rows, block), lambda i: (0, i))
    cache = pl.BlockSpec((slots, heads, dim, block), lambda i: (0, 0, 0, i))
    row = pl.BlockSpec((block, width), lambda i: (i, 0))
    o, gate, k_out, v_out = pl.pallas_call(
        attn_kernel,
        grid=(tokens // block,),
        in_specs=[row, whole(1, width), whole(width, heads, 2 * dim), whole(experts, width), whole(experts, width, cols), lane(1), lane(2), whole(half, 1), cache, cache],
        out_specs=[pl.BlockSpec((2, block, cols), lambda i: (0, i, 0)), lane(2), cache, cache],
        out_shape=[jax.ShapeDtypeStruct((2, tokens, cols), BF16), jax.ShapeDtypeStruct((2, tokens), F32), jax.ShapeDtypeStruct(k_t.shape, BF16), jax.ShapeDtypeStruct(v_t.shape, BF16)],
        scratch_shapes=[pltpu.VMEM((2 * heads, slots, block), F32), pltpu.VMEM((2 * heads, slots * 8, block), F32), pltpu.VMEM((width, 2 * cols), BF16)],
        compiler_params=pltpu.CompilerParams(dimension_semantics=("arbitrary",), vmem_limit_bytes=VMEM_LIMIT),
        name="attention",
    )(x, norm_att.reshape(1, width), w_kv, router_att.T, w_query, positions.reshape(1, tokens), att_ids.T, inv_freq[:, None], k_t, v_t)
    return o, gate, k_out.transpose(3, 0, 1, 2), v_out.transpose(3, 0, 1, 2)


def exchange(cuts, produce, loads, carried, resid_hbm, out_ref, stage, pair_in, held, ring, far_in, full_in, own, resid, sel, resid_sem, swap_sem, ring_sem, d2d_sem):
    rows, width = out_ref.shape
    mine = rows // 2
    chips = lax.axis_size("tp") // 2
    piece = mine // chips
    cw = piece // cuts
    near = cuts // 2
    order = [k for pair in zip(range(near), range(near, cuts)) for k in pair]
    me = lax.axis_index("tp")
    core = lax.rem(me, 2)
    chip = me // 2
    other = 1 - core
    right_chip = lax.rem(chip + 1, chips)
    left_chip = lax.rem(chip + chips - 1, chips)
    far_chip = lax.rem(chip + 2, chips)
    partner = {"tp": chip * 2 + other}
    right = {"tp": right_chip * 2 + core}
    left = {"tp": left_chip * 2 + core}

    barrier = pltpu.get_barrier_semaphore()
    for peer in (partner, right, left):
        pl.semaphore_signal(barrier, inc=1, device_id=peer, device_id_type=MESH)
    for copy in loads:
        copy.start()

    def first_row(c, q):
        return pl.multiple_of(c * mine + q * piece, piece)

    def rows_of(c, q):
        return pl.ds(first_row(c, q), piece)

    resid_copy = pltpu.make_async_copy(resid_hbm.at[rows_of(core, chip)], resid, resid_sem)
    resid_copy.start()
    for copy in loads:
        copy.wait()
    for copy in carried:
        copy.start()
    pending = []

    def send(src, dst, sem, peer):
        copy = pltpu.make_async_remote_copy(src_ref=src, dst_ref=dst, send_sem=sem.at[0], recv_sem=sem.at[1], device_id=peer, device_id_type=MESH)
        copy.start()
        pending.append(copy)
        return copy

    def cut(k):
        return slice(k * cw, (k + 1) * cw)

    def dcut(k):
        return pl.ds(k * cw, cw)

    def swap(slot, q):
        stage[slot] = produce(first_row(other, q), 0, width, sel).astype(BF16)
        if slot == 0:
            pl.semaphore_wait(barrier, 3)
        copy = send(stage.at[slot], pair_in.at[slot], swap_sem.at[slot], partner)
        held[slot] = produce(first_row(core, q), 0, width, sel)
        return copy

    def land(copy, slot):
        copy.wait_recv()
        held[slot] += pair_in[slot].astype(F32)

    far, plain, added = {}, {}, {}
    land(swap(0, far_chip), 0)
    ring[0] = held[0].astype(BF16)
    for k in order:
        far[k] = send(ring.at[0, dcut(k)], far_in.at[dcut(k)], ring_sem.at[k], right if k < near else left)
    land(swap(1, right_chip), 1)
    ring[1, near * cw:] = held[1, near * cw:].astype(BF16)
    for k in range(near, cuts):
        plain[k] = send(ring.at[1, dcut(k)], full_in.at[0, dcut(k)], ring_sem.at[cuts + k], right)
    land(swap(2, left_chip), 2)
    ring[2, :near * cw] = held[2, :near * cw].astype(BF16)
    for k in range(near):
        plain[k] = send(ring.at[2, dcut(k)], full_in.at[1, dcut(k)], ring_sem.at[cuts + k], left)
    for k in order:
        slot = 1 if k < near else 2
        far[k].wait_recv()
        ring[slot, cut(k)] = (held[slot, cut(k)] + far_in[cut(k)].astype(F32)).astype(BF16)
        added[k] = send(ring.at[slot, dcut(k)], full_in.at[slot - 1, dcut(k)], ring_sem.at[2 * cuts + k], right if k < near else left)
    land(swap(3, chip), 3)
    resid_copy.wait()

    own_rows, left_rows, right_rows, far_rows = (rows_of(core, q) for q in (chip, left_chip, right_chip, far_chip))
    to_right, to_left = {}, {}

    def inside(rows_start, k):
        return pl.ds(pl.multiple_of(rows_start + k * cw, cw), cw)

    own_row, left_row, right_row, far_row = (first_row(core, q) for q in (chip, left_chip, right_chip, far_chip))
    for k in order:
        plain[k].wait_recv()
        added[k].wait_recv()
        own[cut(k), :] = (resid[cut(k), :].astype(F32) + (held[3, cut(k), :] + full_in[0, cut(k), :].astype(F32) + full_in[1, cut(k), :].astype(F32))).astype(BF16)
        first, second = ((right, to_right, 3), (left, to_left, 4))[::1 if k < near else -1]
        for peer, table, base in (first, second):
            table[k] = send(own.at[dcut(k)], out_ref.at[inside(own_row, k)], ring_sem.at[base * cuts + k], peer)
    d2d = [send(own, out_ref.at[own_rows], d2d_sem.at[0], partner)]
    out_ref[own_rows, :] = own[...]
    onward = {}
    for k in order:
        if k < near:
            to_right[k].wait_recv()
            onward[k] = send(out_ref.at[inside(left_row, k)], out_ref.at[inside(left_row, k)], ring_sem.at[5 * cuts + k], right)
        else:
            to_left[k].wait_recv()
            onward[k] = send(out_ref.at[inside(right_row, k)], out_ref.at[inside(right_row, k)], ring_sem.at[5 * cuts + k], left)
    for k in range(near, cuts):
        to_right[k].wait_recv()
    d2d.append(send(out_ref.at[left_rows], out_ref.at[left_rows], d2d_sem.at[1], partner))
    for k in range(near):
        to_left[k].wait_recv()
    d2d.append(send(out_ref.at[right_rows], out_ref.at[right_rows], d2d_sem.at[2], partner))
    for i, k in enumerate(order):
        onward[k].wait_recv()
        d2d.append(send(out_ref.at[inside(far_row, k)], out_ref.at[inside(far_row, k)], d2d_sem.at[3 + i], partner))
    for copy in carried:
        copy.wait()
    for copy in d2d:
        copy.wait_recv()
    for copy in pending:
        copy.wait_send()


def load_all(pairs, sem):
    return [pltpu.make_async_copy(src, dst, sem.at[i]) for i, (src, dst) in enumerate(pairs)]


def project_kernel(o_hbm, ids_hbm, gate_hbm, wo_hbm, wg_hbm, wu_hbm, resid_hbm, out_ref, wg_ref, wu_ref, o_ref, ids_ref, gate_ref, wo_ref, load_sem, carry_sem, *rest):
    cols = o_ref.shape[2]
    experts = wo_ref.shape[0] // cols

    def produce(start, col, width, sel):
        block = sel.shape[0]
        total = None
        for j in range(2):
            ids_col = jnp.broadcast_to(ids_ref[j:j + 1, pl.ds(start, block)], (cols, block)).T
            gate_col = jnp.broadcast_to(gate_ref[j:j + 1, pl.ds(start, block)], (cols, block)).T
            o_j = o_ref[j, pl.ds(start, block), :].astype(F32)
            for e in range(experts):
                sel[:, e * cols:(e + 1) * cols] = jnp.where(ids_col == e, o_j, 0.0).astype(BF16)
            projected = jnp.dot(sel[...], wo_ref[:, col:col + width], preferred_element_type=F32)
            scaled = projected * jnp.concatenate([gate_col] * (width // cols), axis=1)
            total = scaled if total is None else total + scaled
        return total

    exchange(4, produce, load_all(((o_hbm, o_ref), (ids_hbm, ids_ref), (gate_hbm, gate_ref), (wo_hbm, wo_ref)), load_sem), load_all(((wg_hbm, wg_ref), (wu_hbm, wu_ref)), carry_sem), resid_hbm, out_ref, *rest)


def combine_kernel(z_hbm, place_hbm, resid_hbm, out_ref, z_ref, place_ref, load_sem, carry_sem, *rest):
    def produce(start, col, width, sel):
        block = sel.shape[0]
        place = [jnp.broadcast_to(place_ref[j:j + 1, pl.ds(start, block)], (block, block)).T for j in range(2)]
        lane = lax.broadcasted_iota(jnp.int32, (block, block), 1).astype(F32)
        for r in range(0, sel.shape[1], block):
            here = lane + float(r)
            sel[:, r:r + block] = jnp.where((place[0] == here) | (place[1] == here), 1.0, 0.0).astype(BF16)
        return jnp.dot(sel[...], z_ref[:, col:col + width], preferred_element_type=F32)

    exchange(4, produce, load_all(((z_hbm, z_ref), (place_hbm, place_ref)), load_sem), [], resid_hbm, out_ref, *rest)


def reduce_call(kernel, operands, depth, resid, collective_id, name, limit, spaces, carried=()):
    rows, width = resid.shape
    piece = rows // lax.axis_size("tp")
    vmem = pl.BlockSpec(memory_space=pltpu.VMEM)
    return pl.pallas_call(
        kernel,
        in_specs=[pl.BlockSpec(memory_space=space) for space in spaces] + [pl.BlockSpec(memory_space=pltpu.HBM)] * len(carried) + [pl.BlockSpec(memory_space=pl.ANY)],
        out_specs=[vmem] * (1 + len(carried)),
        out_shape=[jax.ShapeDtypeStruct(resid.shape, BF16)] + [pltpu.VMEM(a.shape, a.dtype) for a in carried],
        scratch_shapes=[pltpu.VMEM(op.shape, op.dtype) for op in operands] + [
            pltpu.SemaphoreType.DMA((len(operands),)),
            pltpu.SemaphoreType.DMA((2,)),
            pltpu.VMEM((4, piece, width), BF16),
            pltpu.VMEM((4, piece, width), BF16),
            pltpu.VMEM((4, piece, width), F32),
            pltpu.VMEM((3, piece, width), BF16),
            pltpu.VMEM((piece, width), BF16),
            pltpu.VMEM((2, piece, width), BF16),
            pltpu.VMEM((piece, width), BF16),
            pltpu.VMEM((piece, width), BF16),
            pltpu.VMEM((piece, depth), BF16),
            pltpu.SemaphoreType.DMA,
            pltpu.SemaphoreType.DMA((4, 2)),
            pltpu.SemaphoreType.DMA((24, 2)),
            pltpu.SemaphoreType.DMA((13, 2)),
        ],
        compiler_params=pltpu.CompilerParams(collective_id=collective_id, has_side_effects=True, vmem_limit_bytes=limit),
        name=name,
    )(*operands, *carried, resid)


def mlp_kernel(rows, x_hbm, gain_ref, router_ref, ids_ref, wg, wu, wd_hbm, z_hbm, place_ref, x_ref, wd, normed, act, stage, blank, rank_ref, gate_ref, count_ref, flag_ref, sem, z_sem, blank_sem, x_sem):
    tokens, width = x_hbm.shape
    local, _, ffn = wg.shape
    experts = router_ref.shape[0]

    x_copy = pltpu.make_async_copy(x_hbm, x_ref, x_sem)
    x_copy.start()

    def weight(e):
        return pltpu.make_async_copy(wd_hbm.at[e], wd.at[e], sem.at[e])

    ids_row = [ids_ref[j:j + 1, :] for j in range(2)]
    first = lax.axis_index("tp") * local
    local_iota = first + lax.broadcasted_iota(jnp.int32, (8, tokens), 0)
    hit = [(ids_row[j] == local_iota) for j in range(2)]
    member = jnp.where(hit[0] | hit[1], 1.0, 0.0)
    counts = [jnp.sum(member[e:e + 1, :]).astype(jnp.int32) for e in range(local)]
    busiest, most = jnp.int32(0), counts[0]
    for e in range(1, local):
        busiest = jnp.where(counts[e] > most, e, busiest)
        most = jnp.maximum(counts[e], most)

    def nth(i):
        return jnp.where(i == 0, busiest, jnp.where(i - 1 < busiest, i - 1, i))

    flag_ref[0] = 0
    flag_ref[1] = 0
    flag_ref[2] = 0

    def fetch():
        issued = flag_ref[2]

        @pl.when(issued < local)
        def _():
            weight(nth(issued)).start()
            flag_ref[2] = issued + 1

    for _ in range(2):
        fetch()

    step = 128
    blank[...] = jnp.zeros_like(blank)
    x_copy.wait()
    for t in range(0, tokens, step):
        xf = x_ref[t:t + step, :].astype(F32)
        inv = lax.rsqrt(jnp.mean(xf * xf, axis=-1, keepdims=True) + NORM_EPS)
        normed[t:t + step, :] = (xf * inv * gain_ref[...]).astype(BF16)

    logits = lax.dot_general(router_ref[...], normed[...], (((1,), (1,)), ((), ())), preferred_element_type=F32)
    expert_iota = lax.broadcasted_iota(jnp.int32, (experts, tokens), 0)
    picked = [jnp.sum(jnp.where(expert_iota == ids_row[j], logits, 0.0), axis=0, keepdims=True) for j in range(2)]
    top = jnp.maximum(picked[0], picked[1])
    raised = [jnp.exp(p - top) for p in picked]
    gate = [r / (raised[0] + raised[1]) for r in raised]
    gate_ref[...] = jnp.where(hit[0], gate[0], 0.0) + jnp.where(hit[1], gate[1], 0.0)
    tri = jnp.where(lax.broadcasted_iota(jnp.int32, (step, step), 0) <= lax.broadcasted_iota(jnp.int32, (step, step), 1), 1.0, 0.0).astype(BF16)
    running = jnp.zeros((8, 1), F32)
    for t in range(0, tokens, step):
        piece = member[:, t:t + step]
        inside = jnp.dot(piece.astype(BF16), tri, preferred_element_type=F32)
        rank_ref[:, t:t + step] = jnp.where(piece > 0, inside + running - 1.0, -1.0)
        running = running + jnp.sum(piece, axis=1, keepdims=True)

    start = jnp.int32(0)
    place = [jnp.full((1, tokens), -1.0, F32) for _ in range(2)]
    for e in range(local):
        count = counts[e]
        count_ref[e, 0] = count
        count_ref[e, 1] = start
        offset = (start * rows).astype(F32)
        place = [jnp.where(hit[j][e:e + 1, :], rank_ref[e:e + 1, :] + offset, place[j]) for j in range(2)]
        start = start + (count + rows - 1) // rows
    for j in range(2):
        place_ref[j:j + 1, :] = place[j]

    def blank_copy(i):
        return pltpu.make_async_copy(blank, z_hbm.at[pl.ds(pl.multiple_of(i * rows, rows), rows)], blank_sem)

    def z_copy(i, slot, n):
        return pltpu.make_async_copy(stage.at[slot, pl.ds(0, n * rows)], z_hbm.at[pl.ds(pl.multiple_of(i * rows, rows), n * rows)], z_sem.at[slot])

    total_tiles = z_hbm.shape[0] // rows
    used = start

    def blank_start(i, carry):
        blank_copy(i).start()
        return carry

    def tile(e, base, n, z_row):
        size = n * rows
        hits = rank_ref[pl.ds(e, 1), :] == (lax.broadcasted_iota(jnp.int32, (size, tokens), 0) + base).astype(F32)
        gate_col = jnp.sum(jnp.where(hits, gate_ref[pl.ds(e, 1), :], 0.0), axis=1, keepdims=True)
        picked_rows = jnp.dot(jnp.where(hits, 1.0, 0.0).astype(BF16), normed[...], preferred_element_type=F32).astype(BF16)
        for f in range(0, ffn, 512):
            g = jnp.dot(picked_rows, wg[e, :, f:f + 512], preferred_element_type=F32)
            u = jnp.dot(picked_rows, wu[e, :, f:f + 512], preferred_element_type=F32)
            act[:size, f:f + 512] = (jax.nn.silu(g) * u).astype(BF16)

        fetch()

        @pl.when(base == 0)
        def _():
            weight(e).wait()
            fetch()

        down = jnp.dot(act[:size, :], wd[e], preferred_element_type=F32) * gate_col
        slot = n - 1

        @pl.when(flag_ref[slot] == 1)
        def _():
            z_copy(0, slot, n).wait()

        stage[slot, :size, :] = down.astype(BF16)
        z_copy(z_row, slot, n).start()
        flag_ref[slot] = 1
        fetch()

    def expert_step(turn, carry):
        e = nth(turn)
        count = count_ref[e, 0]
        begin = count_ref[e, 1]
        pairs = (count + rows - 1) // (2 * rows)

        def pair_step(i, inner):
            tile(e, i * (2 * rows), 2, begin + 2 * i)
            return inner

        lax.fori_loop(0, pairs, pair_step, 0)

        @pl.when(count > pairs * (2 * rows))
        def _():
            tile(e, pairs * (2 * rows), 1, begin + 2 * pairs)

        @pl.when(count == 0)
        def _():
            weight(e).wait()
            fetch()

        @pl.when(turn == 0)
        def _():
            lax.fori_loop(used, total_tiles, blank_start, 0)

        return carry

    lax.fori_loop(0, local, expert_step, 0)

    def blank_wait(i, carry):
        blank_copy(i).wait()
        return carry

    lax.fori_loop(used, total_tiles, blank_wait, 0)
    for slot in range(2):
        @pl.when(flag_ref[slot] == 1)
        def _():
            z_copy(0, slot, slot + 1).wait()


def experts_mlp(x1, mlp_ids, norm_mlp, router_mlp, w_gate, w_up, w_down, rows=128):
    tokens, width = x1.shape
    local, _, ffn = w_gate.shape
    vmem = pl.BlockSpec(memory_space=pltpu.VMEM)
    hbm = pl.BlockSpec(memory_space=pl.ANY)
    return pl.pallas_call(
        functools.partial(mlp_kernel, rows),
        in_specs=[hbm, vmem, vmem, vmem, vmem, vmem, hbm],
        out_specs=[hbm, vmem],
        out_shape=[jax.ShapeDtypeStruct((2 * tokens + local * rows, width), BF16), pltpu.VMEM((2, tokens), F32)],
        scratch_shapes=[
            pltpu.VMEM((tokens, width), BF16),
            pltpu.VMEM((local, ffn, width), BF16),
            pltpu.VMEM((tokens, width), BF16),
            pltpu.VMEM((2 * rows, ffn), BF16),
            pltpu.VMEM((2, 2 * rows, width), BF16),
            pltpu.VMEM((rows, width), BF16),
            pltpu.VMEM((8, tokens), F32),
            pltpu.VMEM((8, tokens), F32),
            pltpu.SMEM((local, 2), jnp.int32),
            pltpu.SMEM((3,), jnp.int32),
            pltpu.SemaphoreType.DMA((local,)),
            pltpu.SemaphoreType.DMA((2,)),
            pltpu.SemaphoreType.DMA,
            pltpu.SemaphoreType.DMA,
        ],
        compiler_params=pltpu.CompilerParams(vmem_limit_bytes=27 * 1024 * 1024),
        name="experts",
    )(x1, norm_mlp.reshape(1, width), router_mlp.T, mlp_ids.T, pltpu.with_memory_space_constraint(w_gate, pltpu.VMEM), pltpu.with_memory_space_constraint(w_up, pltpu.VMEM), w_down)


def solution(mesh):
    def local_step(x, k_cache, v_cache, positions, att_ids, mlp_ids, norm_att, w_kv, router_att, w_query, w_out, norm_mlp, router_mlp, w_gate, w_up, w_down):
        o, gate, keys_all, values_all = attention(x, k_cache, v_cache, positions, att_ids, norm_att, w_kv, router_att, w_query)
        depth = w_out.shape[0] * w_out.shape[1]
        x_mid, w_gate, w_up = reduce_call(project_kernel, (o, att_ids.T, gate, w_out.reshape(depth, x.shape[1])), depth, x, 0, "project", 27 * 1024 * 1024, (pltpu.HBM,) * 4, (w_gate, w_up))
        z, place = experts_mlp(x_mid, mlp_ids, norm_mlp, router_mlp, w_gate, w_up, w_down)
        x_out, = reduce_call(combine_kernel, (z, pltpu.with_memory_space_constraint(place, pltpu.VMEM)), z.shape[0], x_mid, 1, "combine", 50 * 1024 * 1024, (pltpu.HBM, pltpu.VMEM))
        return x_out, keys_all, values_all

    token_spec = P('dp', None)
    cache_spec = P('dp', None, 'tp', None)
    expert_spec = P('tp', None, None)
    in_specs = (token_spec, cache_spec, cache_spec, P('dp'), token_spec, token_spec, P(), P(None, 'tp', None), P(), P(None, None, 'tp'), P(None, 'tp', None), P(), P(), expert_spec, expert_spec, expert_spec)
    out_specs = (token_spec, cache_spec, cache_spec)
    return jax.shard_map(local_step, mesh=mesh, in_specs=in_specs, out_specs=out_specs, check_vma=False)
```
